256 devices in a mesh: replica: 32 (over y, z), shard: 8 (over x, core).
Axes of the slice: x: 4, y: 4, z: 8, core: 2. Of those that a mesh axis runs over, the one named last changes fastest.
Arguments:
- outer_params: float32 [1024, 4096], P('shard'), may hold values from -6 to 6, as said below
- local_params: bfloat16 [32, 1024, 4096], P('replica', 'shard'), may hold values from -70 to 70
- momentum: float32 [1024, 4096], P('shard'), may hold values from -6 to 6
Outputs:
- params_next: float32 [1024, 4096], P('shard')
- momentum_next: float32 [1024, 4096], P('shard')
- block_scales: float32 [32, 1024], P(None, 'shard')
The draws below stay inside these ranges and needn't reach their ends.
Inputs may be any that keep to these rules, and one draw needn't show every extreme that they name: `outer_params`: outer parameters of order one.
All inputs are finite; a program needn't handle non-finite values.
Results may differ from the reference program's by a relative error of at most 0.005.
Values may be sent and summed in bfloat16 or wider, within the bound.
A program may use at most 64 MiB of HBM per device.

```python
import math
import jax
import jax.numpy as jnp
from jax import lax

D = 4096
BLOCK = 128
ROWS = 1024
WORKERS = 32


def draw_fields(key):
    base_key = jax.random.fold_in(key, 71)
    outer_key = jax.random.fold_in(base_key, 1)
    column_key = jax.random.fold_in(base_key, 2)
    common_key = jax.random.fold_in(base_key, 3)
    noise_key = jax.random.fold_in(base_key, 4)
    level_key = jax.random.fold_in(base_key, 5)
    group_rows = 32
    group_count = (ROWS + group_rows - 1) // group_rows
    raw_levels = jax.random.uniform(level_key, (group_count,), jnp.float32, 0.0, 1.0)
    unit_levels = raw_levels - jnp.max(raw_levels) + 1.0
    row_group = jnp.arange(ROWS, dtype=jnp.int32) // group_rows
    row_scale = 10.0 ** unit_levels[row_group]
    common_part = jnp.clip(jax.random.normal(common_key, (ROWS, D), jnp.float32), -4.0, 4.0)
    noise_part = jnp.clip(jax.random.normal(noise_key, (WORKERS, ROWS, D), jnp.float32), -4.0, 4.0)
    column_scale = jnp.exp(jax.random.uniform(column_key, (D,), jnp.float32, 0.0, math.log(10.0)))
    outer_values = jnp.clip(jax.random.normal(outer_key, (ROWS, D), jnp.float32), -6.0, 6.0)
    deltas = 0.05 * row_scale[:, None] * column_scale[None, :] * (common_part[None] + noise_part)
    return (outer_values, deltas)


def draw_outer_params(key, part):
    outer_values, deltas = draw_fields(key)
    return outer_values


def draw_local_params(key, part):
    outer_values, deltas = draw_fields(key)
    return (outer_values[None] - deltas).astype(jnp.bfloat16)


def block_scale(stream_key, extent, pieces, low, high):
    level = 1.0
    for axis_at, shards_of in pieces:
        draws = jax.random.uniform(jax.random.fold_in(jax.random.fold_in(stream_key, 6), axis_at), (shards_of,), jnp.float32, low / len(pieces), high / len(pieces))
        level = level * jnp.repeat(jnp.exp(draws), extent[axis_at] // shards_of).reshape((-1,) + (1,) * (len(extent) - 1 - axis_at))
    return level


def scatter_about(stream_key, dims, scale, most, pieces=(), kind=jnp.bfloat16):
    values = jax.random.normal(stream_key, dims, jnp.float32) * scale
    if len(pieces) > 0:
        values = block_scale(stream_key, dims, pieces, -0.22, 0.18) * values
    return jnp.clip(values, min=-most, max=most).astype(kind)


def setup_inputs(seed: int = 0) -> dict:
    seeds = jax.random.split(jax.random.key(seed), 4)
    outer_params = draw_outer_params(jax.random.fold_in(seeds[3], 71), 0)
    local_params = draw_local_params(jax.random.fold_in(seeds[3], 71), 0)
    momentum = scatter_about(seeds[2], (ROWS, D), 1.0, 6.0, ((0, 8),), jnp.float32)
    return {"outer_params": outer_params, "local_params": local_params, "momentum": momentum}


epsilon = 1e-06
clip_level = 0.5
outer_rate = 0.7
outer_decay = 0.9
grid_levels = 7.0

def smooth_step(values):
    return values - jnp.sin(2.0 * math.pi * values) / (2.0 * math.pi)

def smooth_round(values):
    return smooth_step(smooth_step(values))

def block_max(values):
    return lax.optimization_barrier(jnp.max(jnp.abs(values).reshape(values.shape[0], D // BLOCK, BLOCK), axis=2))

def reference(outer_params, local_params, momentum):

    def worker_max(running, worker_local):
        deltas = outer_params - worker_local.astype(jnp.float32)
        return (jnp.maximum(running, block_max(deltas)), None)
    absmax, _ = lax.scan(worker_max, jnp.zeros((ROWS, D // BLOCK), jnp.float32), local_params)
    spread_scale = jnp.repeat(absmax + epsilon, BLOCK, axis=1)

    def worker_sum(running, worker_local):
        deltas = outer_params - worker_local.astype(jnp.float32)
        encoded = smooth_round(grid_levels * deltas / spread_scale).astype(jnp.bfloat16)
        return (running + spread_scale * encoded.astype(jnp.float32) / grid_levels, None)
    summed_rows, _ = lax.scan(worker_sum, jnp.zeros((ROWS, D), jnp.float32), local_params)
    gradient = summed_rows / WORKERS
    root_mean = jnp.sqrt(jnp.mean(gradient * gradient) + epsilon)
    factor = jnp.minimum(1.0, clip_level / root_mean)
    clipped = factor * gradient
    momentum_next = outer_decay * momentum + clipped
    params_next = outer_params - outer_rate * (clipped + outer_decay * momentum_next)
    return (params_next, momentum_next, absmax.T)
```

```python
import jax
import jax.numpy as jnp
from jax import lax
from jax.experimental import pallas as pl
from jax.experimental.pallas import tpu as pltpu
from jax.sharding import Mesh
from jax.sharding import PartitionSpec as P

F32, BF16 = jnp.float32, jnp.bfloat16
MESH = pl.DeviceIdType.MESH
BLOCK = 128
AXES = ("y", "z", "x", "core")
SIZES = {"y": 4, "z": 8, "x": 4, "core": 2}
REPLICA = ("y", "z")
SHARD = ("x", "core")
NY, NZ = SIZES["y"], SIZES["z"]
WORKERS = NY * NZ

epsilon = 1e-06
clip_level = 0.5
outer_rate = 0.7
outer_decay = 0.9
grid_levels = 7.0

CURVE = (
    6.579736058540756,
    -12.987862704441794,
    12.207700561043827,
    -6.688877467338575,
    2.372163287039885,
    -0.5163244078344457,
)

Y_STEPS = (2, 1, 3)
Z_FAR = (4, 3, 5, 2, 6, 1, 7)
Z_NEAR = (1, 7, 2, 6, 3, 5, 4)
CELL = tuple((a, b) for a in range(4) for b in range(2) if (a, b) != (0, 0))


def curve(r):
    t = r * r
    p = CURVE[-1]
    for c in CURVE[-2::-1]:
        p = p * t + c
    return (r * t) * p


def smooth_round(v):
    whole = jnp.round(v)
    return whole + curve(curve(v - whole))


def kernel(
    outer_hbm, local_hbm, momentum_hbm, params_ref, momentum_ref, scales_ref,
    outer_v, local_v, momentum_v, maxima, maxima_y, max_own, maxima_z, max_row, max_all,
    inverse, spread, raw_y, partial, total, parts_z, gathered, squares, squares_in,
    load_sem, my_s, my_r, mz_s, mz_r, ma_s, ma_r, raw_s, raw_r, part_s, part_r,
    gz_s, gz_r, gy_s, gy_r, sq_s, sq_r,
):
    y, z = lax.axis_index("y"), lax.axis_index("z")
    x, core = lax.axis_index("x"), lax.axis_index("core")
    at = {"y": y, "z": z, "x": x, "core": core}
    rows, cols = outer_v.shape
    nr, nc = rows // NY, cols // NZ
    per = nc // BLOCK
    entry_count = rows * cols * SIZES["x"] * SIZES["core"]

    def peer(**steps):
        return {k: lax.rem(at[k] + s, SIZES[k]) for k, s in steps.items()}

    def send(src, dst, ss, rs, **steps):
        return pltpu.make_async_remote_copy(
            src_ref=src, dst_ref=dst, send_sem=ss, recv_sem=rs,
            device_id=peer(**steps), device_id_type=MESH,
        )

    def row_of(g):
        return pl.ds(pl.multiple_of(g * nr, nr), nr)

    def col_of(g):
        return pl.ds(pl.multiple_of(g * nc, nc), nc)

    barrier = pltpu.get_barrier_semaphore()
    friends = (
        [dict(y=s) for s in range(1, NY)]
        + [dict(z=s) for s in range(1, NZ)]
        + [dict(x=a, core=b) for a, b in CELL]
    )
    for f in friends:
        pl.semaphore_signal(barrier, inc=1, device_id=peer(**f), device_id_type=MESH)

    loads = []
    for g in range(NY):
        loads.append([
            pltpu.make_async_copy(
                local_hbm.at[0, pl.ds(g * nr, nr)], local_v.at[pl.ds(g * nr, nr)], load_sem.at[g]
            ),
            pltpu.make_async_copy(
                outer_hbm.at[pl.ds(g * nr, nr)], outer_v.at[pl.ds(g * nr, nr)], load_sem.at[NY + g]
            ),
        ])
    for pair in loads:
        for c in pair:
            c.start()
    load_momentum = pltpu.make_async_copy(momentum_hbm, momentum_v, load_sem.at[2 * NY])
    load_momentum.start()

    for g in range(NY):
        for c in loads[g]:
            c.wait()

        def block_max(p, _, g=g):
            blocks = []
            for j in range(per):
                where = (pl.ds(g * nr, nr), pl.ds(pl.multiple_of(p * nc + j * BLOCK, BLOCK), BLOCK))
                blocks.append(jnp.abs(outer_v[where] - local_v[where].astype(F32)))
            stack = jnp.concatenate(blocks, axis=0)
            maxima[g, pl.ds(p, 1), :] = jnp.max(stack.T, axis=0, keepdims=True)
            return 0

        lax.fori_loop(0, NZ, block_max, 0)

    pl.semaphore_wait(barrier, len(friends))

    my = [
        send(maxima.at[lax.rem(y + s, NY)], maxima_y.at[i], my_s.at[i], my_r.at[i], y=s)
        for i, s in enumerate(Y_STEPS)
    ]
    for c in my:
        c.start()

    order = (4, 3, 5, 2, 6, 1, 7, 0)

    def piece_of(i):
        return lax.rem(z + order[i], NZ)

    raw = {}
    for i in range(NZ):
        for k, s in enumerate(Y_STEPS):
            raw[i, k] = send(
                local_v.at[row_of(lax.rem(y + s, NY)), col_of(piece_of(i))],
                raw_y.at[k, i], raw_s.at[k, i], raw_r.at[k, i], y=s,
            )
            raw[i, k].start()

    for c in my:
        c.wait_recv()
    m = maxima[y]
    for i in range(len(Y_STEPS)):
        m = jnp.maximum(m, maxima_y[i])
    max_own[...] = m
    mz = [
        send(max_own, maxima_z.at[i], mz_s.at[i], mz_r.at[i], z=s) for i, s in enumerate(Z_FAR)
    ]
    for c in mz:
        c.start()
    for c in mz:
        c.wait_recv()
    m = max_own[...]
    for i in range(len(Z_FAR)):
        m = jnp.maximum(m, maxima_z[i])
    max_row[...] = m
    ma = [
        send(max_row, max_all.at[y], ma_s.at[i], ma_r.at[i], y=s) for i, s in enumerate(Y_STEPS)
    ]
    for c in ma:
        c.start()
    max_all[y] = m

    inverse_rows = grid_levels / (m + epsilon)
    for p in range(NZ):
        inverse[p] = jnp.broadcast_to(inverse_rows[p : p + 1, :], (BLOCK, BLOCK)).T
    max_own_piece = max_row[pl.ds(z, 1), :] + epsilon
    spread[...] = jnp.broadcast_to(max_own_piece, (BLOCK, BLOCK)).T

    part = {}
    for i in range(NZ):
        p = piece_of(i)
        for k in range(len(Y_STEPS)):
            raw[i, k].wait_recv()

        def encode(j, _, i=i, p=p):
            lanes = pl.ds(pl.multiple_of(j * BLOCK, BLOCK), BLOCK)
            columns = pl.ds(pl.multiple_of(p * nc + j * BLOCK, BLOCK), BLOCK)
            o = outer_v[row_of(y), columns]
            inv = inverse[p, pl.ds(pl.multiple_of(j * nr, nr), nr), :]
            acc = jnp.zeros((nr, BLOCK), F32)
            for w in range(NY):
                local = local_v[row_of(y), columns] if w == 0 else raw_y[w - 1, i, :, lanes]
                v = (o - local.astype(F32)) * inv
                acc += smooth_round(v).astype(BF16).astype(F32)
            if i < NZ - 1:
                partial[i, :, lanes] = acc.astype(BF16)
            else:
                total[:, lanes] = acc
            return 0

        lax.fori_loop(0, per, encode, 0)
        if i < NZ - 1:
            part[i] = send(
                partial.at[i], parts_z.at[i], part_s.at[i], part_r.at[i], z=order[i]
            )
            part[i].start()

    for i in range(NZ - 1):
        part[i].wait_recv()

    sq = jnp.zeros((8, BLOCK), F32)
    for j in range(per):
        lanes = pl.ds(j * BLOCK, BLOCK)
        acc = total[:, lanes]
        for i in range(NZ - 1):
            acc += parts_z[i, :, lanes].astype(F32)
        g = acc * (spread[pl.ds(j * nr, nr), :] * (1.0 / (grid_levels * WORKERS)))
        gathered[y, z, :, lanes] = g.astype(BF16)
        g2 = g * g
        for r in range(nr // 8):
            sq += g2[r * 8 : r * 8 + 8]
    squares[0] = sq

    gz = [
        send(gathered.at[y, z], gathered.at[y, z], gz_s.at[i], gz_r.at[i], z=s)
        for i, s in enumerate(Z_NEAR)
    ]
    qz = [
        send(squares.at[0], squares_in.at[i], sq_s.at[i], sq_r.at[i], z=s)
        for i, s in enumerate(Z_NEAR)
    ]
    gy = {}

    def spread_y(i, source):
        for k, s in enumerate(Y_STEPS):
            ref = gathered.at[y, source]
            gy[i, k] = send(ref, ref, gy_s.at[k, i], gy_r.at[k, i], y=s)
            gy[i, k].start()

    for c, q in zip(gz, qz):
        q.start()
        c.start()
    spread_y(0, z)
    for i, s in enumerate(Z_NEAR):
        source = lax.rem(z + NZ - s, NZ)
        ref = gathered.at[y, source]
        send(ref, ref, gz_s.at[i], gz_r.at[i], z=s).wait_recv()
        spread_y(i + 1, source)

    def add_up(slot, first, copies):
        for c in copies:
            c.wait_recv()
        acc = squares[slot]
        for i in range(len(copies)):
            acc += squares_in[first + i]
        squares[slot + 1] = acc

    add_up(0, 0, qz)
    qy = [
        send(squares.at[1], squares_in.at[7 + i], sq_s.at[7 + i], sq_r.at[7 + i], y=s)
        for i, s in enumerate(Y_STEPS)
    ]
    for q in qy:
        q.start()
    add_up(1, 7, qy)
    qc = [
        send(squares.at[2], squares_in.at[10 + i], sq_s.at[10 + i], sq_r.at[10 + i], x=a, core=b)
        for i, (a, b) in enumerate(CELL)
    ]
    for q in qc:
        q.start()
    add_up(2, 10, qc)
    square_total = jnp.sum(squares[3], axis=(0, 1), keepdims=True)
    root_mean = jnp.sqrt(square_total / entry_count + epsilon)
    factor = jnp.minimum(1.0, clip_level / root_mean)

    for c in ma:
        c.wait_recv()
    lane = lax.broadcasted_iota(jnp.int32, (NZ, BLOCK), 1)
    for j in range(per):
        out = jnp.zeros((NZ, BLOCK), F32)
        for g in range(NY):
            rolled = pltpu.roll(max_all[g], (g - j) * nr % BLOCK, 1)
            out = jnp.where((lane >= g * nr) & (lane < g * nr + nr), rolled, out)
        scales_ref[pl.ds(j, NZ, stride=per), :] = out

    load_momentum.wait()
    for i in range(NZ):
        source = z if i == 0 else lax.rem(z + NZ - Z_NEAR[i - 1], NZ)
        for k in range(NY):
            group = y if k == 0 else lax.rem(y + NY - Y_STEPS[k - 1], NY)
            if k > 0:
                ref = gathered.at[group, source]
                send(ref, ref, gy_s.at[k - 1, i], gy_r.at[k - 1, i], y=1).wait_recv()

            where = (row_of(group), col_of(source))
            clipped = factor * gathered[group, source].astype(F32)
            after = outer_decay * momentum_v[where] + clipped
            momentum_ref[where] = after
            params_ref[where] = outer_v[where] - outer_rate * (clipped + outer_decay * after)

    for c in my + mz + ma + gz + qz + qy + qc:
        c.wait_send()
    for group in (raw, part, gy):
        for c in group.values():
            c.wait_send()


def per_device(outer_params, local_params, momentum):
    rows, cols = outer_params.shape
    nr, nc = rows // NY, cols // NZ
    vmem = pltpu.VMEM
    dma = pltpu.SemaphoreType.DMA
    return pl.pallas_call(
        kernel,
        out_shape=(
            jax.ShapeDtypeStruct((rows, cols), F32),
            jax.ShapeDtypeStruct((rows, cols), F32),
            jax.ShapeDtypeStruct((cols // BLOCK, rows), F32),
        ),
        in_specs=[pl.BlockSpec(memory_space=pl.ANY)] * 3,
        out_specs=[pl.BlockSpec(memory_space=pltpu.VMEM)] * 3,
        scratch_shapes=[
            vmem((rows, cols), F32),
            vmem((rows, cols), BF16),
            vmem((rows, cols), F32),
            vmem((NY, NZ, BLOCK), F32),
            vmem((NY - 1, NZ, BLOCK), F32),
            vmem((NZ, BLOCK), F32),
            vmem((NZ - 1, NZ, BLOCK), F32),
            vmem((NZ, BLOCK), F32),
            vmem((NY, NZ, BLOCK), F32),
            vmem((NZ, BLOCK, BLOCK), F32),
            vmem((BLOCK, BLOCK), F32),
            vmem((NY - 1, NZ, nr, nc), BF16),
            vmem((NZ - 1, nr, nc), BF16),
            vmem((nr, nc), F32),
            vmem((NZ - 1, nr, nc), BF16),
            vmem((NY, NZ, nr, nc), BF16),
            vmem((4, 8, BLOCK), F32),
            vmem((17, 8, BLOCK), F32),
            dma((2 * NY + 1,)),
            dma((3,)), dma((3,)), dma((7,)), dma((7,)), dma((3,)), dma((3,)),
            dma((3, NZ)), dma((3, NZ)), dma((7,)), dma((7,)),
            dma((7,)), dma((7,)), dma((3, NZ)), dma((3, NZ)), dma((17,)), dma((17,)),
        ],
        compiler_params=pltpu.CompilerParams(collective_id=0, has_side_effects=True),
        name="outer_step",
    )(outer_params, local_params, momentum)


def solution(mesh):
    finer = Mesh(mesh.devices.reshape([SIZES[a] for a in AXES]), AXES)
    placed = (P(SHARD, None), P(REPLICA, SHARD, None), P(SHARD, None))
    return jax.shard_map(
        per_device,
        mesh=finer,
        in_specs=placed,
        out_specs=(P(SHARD, None), P(SHARD, None), P(None, SHARD)),
        check_vma=False,
    )
```

```python
import jax
import jax.numpy as jnp
from jax import lax
from jax.experimental import pallas as pl
from jax.experimental.pallas import tpu as pltpu
from jax.sharding import Mesh
from jax.sharding import PartitionSpec as P

F32, BF16 = jnp.float32, jnp.bfloat16
MESH = pl.DeviceIdType.MESH
BLOCK = 128
AXES = ("y", "z", "x", "core")
SIZES = {"y": 4, "z": 8, "x": 4, "core": 2}
REPLICA = ("y", "z")
SHARD = ("x", "core")
NY, NZ = SIZES["y"], SIZES["z"]
WORKERS = NY * NZ

epsilon = 1e-06
clip_level = 0.5
outer_rate = 0.7
outer_decay = 0.9
grid_levels = 7.0

CURVE = (
    6.579736058540756,
    -12.987862704441794,
    12.207700561043827,
    -6.688877467338575,
    2.372163287039885,
    -0.5163244078344457,
)

Y_STEPS = (2, 1, 3)
Z_FAR = (4, 3, 5, 2, 6, 1, 7)
Z_NEAR = (1, 7, 2, 6, 3, 5, 4)
CELL = tuple((a, b) for a in range(4) for b in range(2) if (a, b) != (0, 0))


def curve(r):
    t = r * r
    p = CURVE[-1]
    for c in CURVE[-2::-1]:
        p = p * t + c
    return (r * t) * p


def smooth_round(v):
    whole = jnp.round(v)
    return whole + curve(curve(v - whole))


def eighth_power(s):
    t = s * s
    return (s * jnp.abs(s)) * t * (t * t)


def eighth_root(c):
    c = c.astype(F32)
    size = jnp.exp(0.125 * jnp.log(jnp.maximum(jnp.abs(c), 1e-37)))
    return jnp.where(c < 0.0, -size, size)


def kernel(
    outer_hbm, local_hbm, momentum_hbm, params_ref, momentum_ref, scales_ref,
    outer_v, local_v, momentum_v, maxima, maxima_y, max_own, maxima_z, max_all,
    inverse, spread, raw_y, partial, total, parts_z, gathered, squares, squares_in,
    load_sem, my_s, my_r, mz_s, mz_r, ma_s, ma_r, raw_s, raw_r, part_s, part_r,
    gz_s, gz_r, gy_s, gy_r, sq_s, sq_r,
):
    y, z = lax.axis_index("y"), lax.axis_index("z")
    x, core = lax.axis_index("x"), lax.axis_index("core")
    at = {"y": y, "z": z, "x": x, "core": core}
    rows, cols = outer_v.shape
    nr, nc = rows // NY, cols // NZ
    per = nc // BLOCK
    nb = cols // BLOCK
    entry_count = rows * cols * SIZES["x"] * SIZES["core"]
    lane = lax.broadcasted_iota(jnp.int32, (8, BLOCK), 1)

    def peer(**steps):
        return {k: lax.rem(at[k] + s, SIZES[k]) for k, s in steps.items()}

    def send(src, dst, ss, rs, **steps):
        return pltpu.make_async_remote_copy(
            src_ref=src, dst_ref=dst, send_sem=ss, recv_sem=rs,
            device_id=peer(**steps), device_id_type=MESH,
        )

    def row_of(g):
        return pl.ds(pl.multiple_of(g * nr, nr), nr)

    def col_of(g):
        return pl.ds(pl.multiple_of(g * nc, nc), nc)

    def aligned(n):
        return pl.ds(pl.multiple_of(n * BLOCK, BLOCK), BLOCK)

    barrier = pltpu.get_barrier_semaphore()
    friends = (
        [dict(y=s) for s in range(1, NY)]
        + [dict(z=s) for s in range(1, NZ)]
        + [dict(x=a, core=b) for a, b in CELL]
    )
    for f in friends:
        pl.semaphore_signal(barrier, inc=1, device_id=peer(**f), device_id_type=MESH)

    load_local = pltpu.make_async_copy(local_hbm.at[0], local_v, load_sem.at[NY])
    load_momentum = pltpu.make_async_copy(momentum_hbm, momentum_v, load_sem.at[NY + 1])
    load_outer = [
        pltpu.make_async_copy(
            outer_hbm.at[pl.ds(g * nr, nr)], outer_v.at[pl.ds(g * nr, nr)], load_sem.at[g]
        )
        for g in range(NY)
    ]
    for c in [load_local, *load_outer, load_momentum]:
        c.start()
    load_local.wait()
    pl.semaphore_wait(barrier, len(friends))

    order = (4, 3, 5, 2, 6, 1, 7, 0)
    pieces = [lax.rem(z + o, NZ) for o in order]
    raw = {}

    def send_raw(i):
        for k, s in enumerate(Y_STEPS):
            raw[i, k] = send(
                local_v.at[row_of(lax.rem(y + s, NY)), col_of(pieces[i])],
                raw_y.at[k, i], raw_s.at[k, i], raw_r.at[k, i], y=s,
            )
            raw[i, k].start()

    send_raw(0)
    send_raw(1)

    for g in range(NY):
        load_outer[g].wait()

        def block_max(b, acc, g=g):
            out = acc
            for r in range(nr // 8):
                where = (pl.ds(g * nr + r * 8, 8), aligned(b))
                deltas = outer_v[where] - local_v[where].astype(F32)
                most = jnp.max(jnp.abs(deltas), axis=1, keepdims=True)
                out = jnp.where(lane == r * nb + b, most, out)
            return out

        maxima[g] = lax.fori_loop(0, nb, block_max, jnp.zeros((8, BLOCK), F32), unroll=16)

    my = [
        send(maxima.at[lax.rem(y + s, NY)], maxima_y.at[i], my_s.at[i], my_r.at[i], y=s)
        for i, s in enumerate(Y_STEPS)
    ]
    for c in my:
        c.start()
    for i in range(2, NZ):
        send_raw(i)
    for c in my:
        c.wait_recv()
    m = maxima[y]
    for i in range(len(Y_STEPS)):
        m = jnp.maximum(m, maxima_y[i])
    max_own[...] = m
    mz = [
        send(max_own, maxima_z.at[i], mz_s.at[i], mz_r.at[i], z=s) for i, s in enumerate(Z_FAR)
    ]
    for c in mz:
        c.start()
    for c in mz:
        c.wait_recv()
    m = max_own[...]
    for i in range(len(Z_FAR)):
        m = jnp.maximum(m, maxima_z[i])
    max_all[y] = m
    ma = [
        send(max_all.at[y], max_all.at[y], ma_s.at[i], ma_r.at[i], y=s)
        for i, s in enumerate(Y_STEPS)
    ]
    for c in ma:
        c.start()

    scale = m + epsilon
    inverse_scale = grid_levels / scale
    for b in range(nb):
        for r in range(nr // 8):
            n = r * nb + b
            inverse[b, pl.ds(r * 8, 8), :] = jnp.broadcast_to(
                inverse_scale[:, n : n + 1], (8, BLOCK)
            )

    part = {}
    for i in range(NZ):
        p = pieces[i]
        for k in range(len(Y_STEPS)):
            raw[i, k].wait_recv()

        def encode(j, _, i=i, p=p):
            lanes = aligned(j)
            columns = aligned(p * per + j)
            o = outer_v[row_of(y), columns]
            inv = inverse[p * per + j]
            acc = jnp.zeros((nr, BLOCK), F32)
            for w in range(NY):
                local = local_v[row_of(y), columns] if w == 0 else raw_y[w - 1, i, :, lanes]
                v = (o - local.astype(F32)) * inv
                acc += smooth_round(v).astype(BF16).astype(F32)
            if i < NZ - 1:
                partial[i, :, lanes] = eighth_power(acc).astype(BF16)
            else:
                total[:, lanes] = acc
            return 0

        lax.fori_loop(0, per, encode, 0)
        if i < NZ - 1:
            part[i] = send(
                partial.at[i], parts_z.at[i], part_s.at[i], part_r.at[i], z=order[i]
            )
            part[i].start()

    for i in range(NZ - 1):
        part[i].wait_recv()

    sq = jnp.zeros((8, BLOCK), F32)
    for j in range(per):
        lanes = pl.ds(j * BLOCK, BLOCK)
        acc = total[:, lanes]
        for i in range(NZ - 1):
            acc += eighth_root(parts_z[i, :, lanes])
        gathered[y, z, :, lanes] = eighth_power(acc).astype(BF16)
        g = acc / inverse[z * per + j] * (1.0 / WORKERS)
        g2 = g * g
        for r in range(nr // 8):
            sq += g2[r * 8 : r * 8 + 8]
    squares[0] = sq

    qc = [
        send(squares.at[0], squares_in.at[i], sq_s.at[i], sq_r.at[i], x=a, core=b)
        for i, (a, b) in enumerate(CELL)
    ]
    gz = [
        send(gathered.at[y, z], gathered.at[y, z], gz_s.at[i], gz_r.at[i], z=s)
        for i, s in enumerate(Z_NEAR)
    ]
    gy = {}

    def spread_y(i, source):
        for k, s in enumerate(Y_STEPS):
            ref = gathered.at[y, source]
            gy[i, k] = send(ref, ref, gy_s.at[k, i], gy_r.at[k, i], y=s)
            gy[i, k].start()

    def add_up(slot, first, copies):
        for c in copies:
            c.wait_recv()
        acc = squares[slot]
        for i in range(len(copies)):
            acc += squares_in[first + i]
        squares[slot + 1] = acc

    def pass_on(i):
        source = lax.rem(z + NZ - Z_NEAR[i], NZ)
        ref = gathered.at[y, source]
        send(ref, ref, gz_s.at[i], gz_r.at[i], z=Z_NEAR[i]).wait_recv()
        spread_y(i + 1, source)

    for c in gz:
        c.start()
    for c in qc:
        c.start()
    spread_y(0, z)

    for c in ma:
        c.wait_recv()
    for g in range(NY):
        group_scale = (max_all[g] + epsilon) * (1.0 / (grid_levels * WORKERS))
        for b in range(nb):
            for r in range(nr // 8):
                n = r * nb + b
                spread[b, pl.ds(g * nr + r * 8, 8), :] = jnp.broadcast_to(
                    group_scale[:, n : n + 1], (8, BLOCK)
                )
        if g == 0:
            pass_on(0)
    add_up(0, 0, qc)
    qy = [
        send(squares.at[1], squares_in.at[7 + i], sq_s.at[7 + i], sq_r.at[7 + i], y=s)
        for i, s in enumerate(Y_STEPS)
    ]
    for q in qy:
        q.start()
    pass_on(1)
    pass_on(2)
    pass_on(3)
    add_up(1, 7, qy)
    qz = [
        send(squares.at[2], squares_in.at[10 + i], sq_s.at[10 + i], sq_r.at[10 + i], z=s)
        for i, s in enumerate(Z_NEAR)
    ]
    for q in qz:
        q.start()
    for i in range(4, NZ - 1):
        pass_on(i)

    stack = []
    for g in range(NY):
        for r in range(nr // 8):
            turned = max_all[g] if r == 0 else pltpu.roll(max_all[g], BLOCK - r * nb, 1)
            stack.append(turned)
    scales_ref[...] = jnp.concatenate(stack, axis=0).T[:nb]

    load_momentum.wait()
    add_up(2, 10, qz)
    square_total = jnp.sum(squares[3], axis=(0, 1), keepdims=True)
    root_mean = jnp.sqrt(square_total / entry_count + epsilon)
    factor = jnp.minimum(1.0, clip_level / root_mean)

    for i in range(NZ):
        source = z if i == 0 else lax.rem(z + NZ - Z_NEAR[i - 1], NZ)
        for k in range(NY):
            group = y if k == 0 else lax.rem(y + NY - Y_STEPS[k - 1], NY)
            if k > 0:
                ref = gathered.at[group, source]
                send(ref, ref, gy_s.at[k - 1, i], gy_r.at[k - 1, i], y=1).wait_recv()

            def outer_step(j, _, source=source, group=group):
                where = (row_of(group), aligned(source * per + j))
                sums = eighth_root(gathered[group, source, :, aligned(j)])
                clipped = sums * spread[source * per + j, row_of(group)] * factor
                after = outer_decay * momentum_v[where] + clipped
                momentum_ref[where] = after
                params_ref[where] = outer_v[where] - outer_rate * (clipped + outer_decay * after)
                return 0

            lax.fori_loop(0, per, outer_step, 0, unroll=True)

    for c in my + mz + ma + gz + qz + qy + qc:
        c.wait_send()
    for copies in (raw, part, gy):
        for c in copies.values():
            c.wait_send()


def per_device(outer_params, local_params, momentum):
    rows, cols = outer_params.shape
    nr, nc = rows // NY, cols // NZ
    vmem = pltpu.VMEM
    dma = pltpu.SemaphoreType.DMA
    return pl.pallas_call(
        kernel,
        out_shape=(
            jax.ShapeDtypeStruct((rows, cols), F32),
            jax.ShapeDtypeStruct((rows, cols), F32),
            jax.ShapeDtypeStruct((cols // BLOCK, rows), F32),
        ),
        in_specs=[pl.BlockSpec(memory_space=pltpu.HBM)] * 3,
        out_specs=[pl.BlockSpec(memory_space=pltpu.VMEM)] * 3,
        scratch_shapes=[
            vmem((rows, cols), F32),
            vmem((rows, cols), BF16),
            vmem((rows, cols), F32),
            vmem((NY, 8, BLOCK), F32),
            vmem((NY - 1, 8, BLOCK), F32),
            vmem((8, BLOCK), F32),
            vmem((NZ - 1, 8, BLOCK), F32),
            vmem((NY, 8, BLOCK), F32),
            vmem((cols // BLOCK, nr, BLOCK), F32),
            vmem((cols // BLOCK, rows, BLOCK), F32),
            vmem((NY - 1, NZ, nr, nc), BF16),
            vmem((NZ - 1, nr, nc), BF16),
            vmem((nr, nc), F32),
            vmem((NZ - 1, nr, nc), BF16),
            vmem((NY, NZ, nr, nc), BF16),
            vmem((4, 8, BLOCK), F32),
            vmem((17, 8, BLOCK), F32),
            dma((NY + 2,)),
            dma((3,)), dma((3,)), dma((7,)), dma((7,)), dma((3,)), dma((3,)),
            dma((3, NZ)), dma((3, NZ)), dma((7,)), dma((7,)),
            dma((7,)), dma((7,)), dma((3, NZ)), dma((3, NZ)), dma((17,)), dma((17,)),
        ],
        compiler_params=pltpu.CompilerParams(
            collective_id=0, has_side_effects=True, vmem_limit_bytes=32 * 1024 * 1024
        ),
        name="outer_step",
    )(*[pltpu.with_memory_space_constraint(a, pltpu.HBM) for a in (outer_params, local_params, momentum)])


def solution(mesh):
    finer = Mesh(mesh.devices.reshape([SIZES[a] for a in AXES]), AXES)
    placed = (P(SHARD, None), P(REPLICA, SHARD, None), P(SHARD, None))
    return jax.shard_map(
        per_device,
        mesh=finer,
        in_specs=placed,
        out_specs=(P(SHARD, None), P(SHARD, None), P(None, SHARD)),
        check_vma=False,
    )
```

```python
import jax
import jax.numpy as jnp
from jax import lax
from jax.experimental import pallas as pl
from jax.experimental.pallas import tpu as pltpu
from jax.sharding import Mesh
from jax.sharding import PartitionSpec as P

F32, BF16 = jnp.float32, jnp.bfloat16
MESH = pl.DeviceIdType.MESH
BLOCK = 128
AXES = ("y", "z", "x", "core")
SIZES = {"y": 4, "z": 8, "x": 4, "core": 2}
REPLICA = ("y", "z")
SHARD = ("x", "core")
NY, NZ = SIZES["y"], SIZES["z"]
WORKERS = NY * NZ

epsilon = 1e-06
clip_level = 0.5
outer_rate = 0.7
outer_decay = 0.9
grid_levels = 7.0

CURVE = (
    6.579736058540756,
    -12.987862704441794,
    12.207700561043827,
    -6.688877467338575,
    2.372163287039885,
    -0.5163244078344457,
)

Y_STEPS = (2, 1, 3)
Z_FAR = (4, 3, 5, 2, 6, 1, 7)
Z_NEAR = (1, 7, 2, 6, 3, 5, 4)
CELL = tuple((a, b) for a in range(4) for b in range(2) if (a, b) != (0, 0))


def curve(r):
    t = r * r
    p = CURVE[-1]
    for c in CURVE[-2::-1]:
        p = p * t + c
    return (r * t) * p


def smooth_round(v):
    whole = jnp.round(v)
    return whole + curve(curve(v - whole))


def eighth_power(s):
    t = s * s
    return (s * jnp.abs(s)) * t * (t * t)


def eighth_root(c):
    c = c.astype(F32)
    size = jnp.exp(0.125 * jnp.log(jnp.maximum(jnp.abs(c), 1e-37)))
    return jnp.where(c < 0.0, -size, size)


def kernel(
    outer_hbm, local_hbm, momentum_hbm, gradient_ref, factor_ref, scales_ref, outer_v, momentum_v,
    local_v, maxima, maxima_y, max_own, maxima_z, max_all,
    inverse, inverse_z, spread, raw_y, raw_z, partial, partial_y, total, parts_z, parts_y, gathered,
    squares, squares_in, load_sem, one_s, one_r, raw_r, gz_r, gy_r, gh_r,
):
    y, z = lax.axis_index("y"), lax.axis_index("z")
    x, core = lax.axis_index("x"), lax.axis_index("core")
    at = {"y": y, "z": z, "x": x, "core": core}
    rows, cols = outer_v.shape
    nr, nc = rows // NY, cols // NZ
    per = nc // BLOCK
    near = per - 1
    nb = cols // BLOCK
    entry_count = rows * cols * SIZES["x"] * SIZES["core"]
    lane = lax.broadcasted_iota(jnp.int32, (8, BLOCK), 1)
    MY, MZ, MA, RY, RZ, PZ, PY, GZ, GO, GY, GH, QC, QY, QZ = range(14)

    def peer(**steps):
        return {k: lax.rem(at[k] + s, SIZES[k]) for k, s in steps.items()}

    def send(src, dst, ss, rs, **steps):
        pltpu.make_async_remote_copy(
            src_ref=src, dst_ref=dst, send_sem=ss, recv_sem=rs,
            device_id=peer(**steps), device_id_type=MESH,
        ).start()

    def all_of(ref, ss, rs):
        return pltpu.make_async_remote_copy(
            src_ref=ref, dst_ref=ref, send_sem=ss, recv_sem=rs,
            device_id=peer(y=1), device_id_type=MESH,
        )

    def landed(ref, sem):
        all_of(ref, one_s.at[0], sem).wait_recv()

    def row_of(g):
        return pl.ds(pl.multiple_of(g * nr, nr), nr)

    def aligned(n, count=1):
        return pl.ds(pl.multiple_of(n * BLOCK, BLOCK), count * BLOCK)

    barrier = pltpu.get_barrier_semaphore()
    friends = (
        [dict(y=s) for s in range(1, NY)]
        + [dict(z=s) for s in range(1, NZ)]
        + [dict(x=a, core=b) for a, b in CELL]
    )
    for f in friends:
        pl.semaphore_signal(barrier, inc=1, device_id=peer(**f), device_id_type=MESH)

    load_momentum = pltpu.make_async_copy(momentum_hbm, momentum_v, load_sem.at[2, 0])
    loads = [
        pltpu.make_async_copy(src.at[pl.ds(g * nr, nr)], dst.at[pl.ds(g * nr, nr)], load_sem.at[k, g])
        for g in range(NY)
        for k, (src, dst) in enumerate(((local_hbm.at[0], local_v), (outer_hbm, outer_v)))
    ]
    for c in [*loads, load_momentum]:
        c.start()

    lasts = jnp.zeros((8, BLOCK), F32)
    for g in range(NY):
        loads[2 * g].wait()
        loads[2 * g + 1].wait()

        def block_max(p, acc, g=g):
            out, lasts = acc
            for j in range(per):
                for r in range(nr // 8):
                    where = (pl.ds(g * nr + r * 8, 8), aligned(p * per + j))
                    deltas = outer_v[where] - local_v[where].astype(F32)
                    most = jnp.max(jnp.abs(deltas), axis=1, keepdims=True)
                    out = jnp.where(lane == r * nb + p * per + j, most, out)
                    if j == near:
                        lasts = jnp.where(lane == p * (rows // 8) + g * (nr // 8) + r, most, lasts)
            return out, lasts

        maxima[g], lasts = lax.fori_loop(
            0, NZ, block_max, (jnp.zeros((8, BLOCK), F32), lasts), unroll=4
        )
    maxima[NY] = lasts

    pl.semaphore_wait(barrier, len(friends))

    order = (4, 3, 5, 2, 6, 1, 7, 0)
    pieces = [lax.rem(z + o, NZ) for o in order]

    def send_raw_y(i):
        for k, s in enumerate(Y_STEPS):
            send(
                local_v.at[row_of(lax.rem(y + s, NY)), aligned(pieces[i] * per, near)],
                raw_y.at[k, i], one_s.at[RY], raw_r.at[i], y=s,
            )

    def send_raw_z(i):
        s = Z_FAR[i]
        send(
            local_v.at[:, aligned(lax.rem(z + s, NZ) * per + near)],
            raw_z.at[i], one_s.at[RZ], one_r.at[RZ], z=s,
        )

    for i, s in enumerate(Y_STEPS):
        send(maxima.at[lax.rem(y + s, NY)], maxima_y.at[i, 0], one_s.at[MY], one_r.at[MY], y=s)
        send(maxima.at[NY], maxima_y.at[i, 1], one_s.at[MY], one_r.at[MY], y=s)
    for i in range(NZ):
        send_raw_y(i)
        if i < 2:
            send_raw_z(i)
    landed(maxima_y, one_r.at[MY])
    for k, row in enumerate((y, NY)):
        m = maxima[row]
        for i in range(len(Y_STEPS)):
            m = jnp.maximum(m, maxima_y[i, k])
        max_own[k] = m
    for i, s in enumerate(Z_FAR):
        send(max_own, maxima_z.at[i], one_s.at[MZ], one_r.at[MZ], z=s)
    for i in range(2, NZ - 1):
        send_raw_z(i)
    landed(maxima_z, one_r.at[MZ])
    m, lasts = max_own[0], max_own[1]
    for i in range(len(Z_FAR)):
        m = jnp.maximum(m, maxima_z[i, 0])
        lasts = jnp.maximum(lasts, maxima_z[i, 1])
    max_all[y] = m
    for s in Y_STEPS:
        send(max_all.at[y], max_all.at[y], one_s.at[MA], one_r.at[MA], y=s)

    inverse_scale = grid_levels / (m + epsilon)
    for b in range(nb):
        for r in range(nr // 8):
            n = r * nb + b
            inverse[b, pl.ds(r * 8, 8), :] = jnp.broadcast_to(
                inverse_scale[:, n : n + 1], (8, BLOCK)
            )

    def encoded(o, local, inv):
        v = (o - local.astype(F32)) * inv
        return smooth_round(v).astype(BF16).astype(F32)

    def along_y(i):
        p = pieces[i]
        landed(raw_y.at[:, i], raw_r.at[i])

        def encode(j, _):
            lanes = aligned(j)
            columns = aligned(p * per + j)
            o = outer_v[row_of(y), columns]
            inv = inverse[p * per + j]
            acc = encoded(o, local_v[row_of(y), columns], inv)
            for k in range(len(Y_STEPS)):
                acc += encoded(o, raw_y[k, i, :, lanes], inv)
            if i < NZ - 1:
                partial[i, :, lanes] = eighth_power(acc).astype(BF16)
            else:
                total[:, lanes] = acc
            return 0

        lax.fori_loop(0, near, encode, 0)
        if i < NZ - 1:
            send(partial.at[i], parts_z.at[i], one_s.at[PZ], one_r.at[PZ], z=order[i])

    def along_z():
        landed(raw_z, one_r.at[RZ])
        last = z * per + near
        turned = pltpu.roll(grid_levels / (lasts + epsilon), BLOCK - z * (rows // 8), 1)
        for r in range(rows // 8):
            inverse_z[pl.ds(r * 8, 8), :] = jnp.broadcast_to(turned[:, r : r + 1], (8, BLOCK))

        def encode(g, _):
            inv = inverse_z[row_of(g), :]
            o = outer_v[row_of(g), aligned(last)]
            acc = encoded(o, local_v[row_of(g), aligned(last)], inv)
            for k in range(NZ - 1):
                acc += encoded(o, raw_z[k, row_of(g), :], inv)
            partial_y[g] = eighth_power(acc).astype(BF16)

            @pl.when(g == y)
            def _():
                total[:, pl.ds(near * BLOCK, BLOCK)] = acc

            return 0

        lax.fori_loop(0, NY, encode, 0)
        for k, s in enumerate(Y_STEPS):
            send(partial_y.at[lax.rem(y + s, NY)], parts_y.at[k], one_s.at[PY], one_r.at[PY], y=s)

    for i in range(5):
        along_y(i)
    along_z()
    for i in range(5, NZ):
        along_y(i)
    landed(parts_z, one_r.at[PZ])
    landed(parts_y, one_r.at[PY])

    sq = jnp.zeros((8, BLOCK), F32)
    for j in range(per):
        lanes = pl.ds(j * BLOCK, BLOCK)
        acc = total[:, lanes]
        if j < near:
            for i in range(NZ - 1):
                acc += eighth_root(parts_z[i, :, lanes])
        else:
            for i in range(NY - 1):
                acc += eighth_root(parts_y[i])
        gathered[y, z, j] = eighth_power(acc).astype(BF16)
        g = acc / inverse[z * per + j] * (1.0 / WORKERS)
        g2 = g * g
        for r in range(nr // 8):
            sq += g2[r * 8 : r * 8 + 8]
    squares[0] = sq

    most = pl.ds(0, near)

    def pass_on(i):
        source = lax.rem(z + NZ - Z_NEAR[i], NZ)
        ref = gathered.at[y, source, most]
        landed(ref, gz_r.at[i])
        for s in Y_STEPS:
            send(ref, ref, one_s.at[GY], gy_r.at[i], y=s)

    def pass_last(i):
        ref = gathered.at[:, z, near]
        send(ref, ref, one_s.at[GH], gh_r.at[i], z=Z_FAR[i])

    def add_up(slot, first, count, sem):
        landed(squares_in.at[pl.ds(first, count)], sem)
        acc = squares[slot]
        for i in range(count):
            acc += squares_in[first + i]
        squares[slot + 1] = acc

    for i, s in enumerate(Z_NEAR):
        send(squares.at[0], squares_in.at[i], one_s.at[QZ], one_r.at[QZ], z=s)
    ref = gathered.at[y, z, most]
    for i, s in enumerate(Z_NEAR):
        send(ref, ref, one_s.at[GZ], gz_r.at[i], z=s)
    ref = gathered.at[y, z]
    for s in Y_STEPS:
        send(ref, ref, one_s.at[GO], one_r.at[GO], y=s)

    def spread_scale(g):
        group_scale = (max_all[g] + epsilon) * (1.0 / (grid_levels * WORKERS))
        for b in range(nb):
            for r in range(nr // 8):
                n = r * nb + b
                spread[b, pl.ds(g * nr + r * 8, 8), :] = jnp.broadcast_to(
                    group_scale[:, n : n + 1], (8, BLOCK)
                )

    landed(maxima_y.at[:, 0], one_r.at[MA])
    spread_scale(0)
    spread_scale(1)
    pass_on(0)
    pass_on(1)
    landed(raw_z.at[pl.ds(0, NY - 1)], one_r.at[GO])
    for i in range(NZ - 1):
        pass_last(i)
    add_up(0, 0, 7, one_r.at[QZ])
    for i, s in enumerate(Y_STEPS):
        send(squares.at[1], squares_in.at[7 + i], one_s.at[QY], one_r.at[QY], y=s)
    pass_on(2)
    spread_scale(2)
    pass_on(3)
    spread_scale(3)
    pass_on(4)
    add_up(1, 7, 3, one_r.at[QY])
    for i, (a, b) in enumerate(CELL):
        send(squares.at[2], squares_in.at[10 + i], one_s.at[QC], one_r.at[QC], x=a, core=b)
    pass_on(5)
    pass_on(6)

    stack = []
    for g in range(NY):
        for r in range(nr // 8):
            turned = max_all[g] if r == 0 else pltpu.roll(max_all[g], BLOCK - r * nb, 1)
            stack.append(turned)
    scales_ref[...] = jnp.concatenate(stack, axis=0).T[:nb]

    for i in range(NZ):
        source = z if i == 0 else lax.rem(z + NZ - Z_NEAR[i - 1], NZ)
        if i > 0:
            landed(raw_y.at[:, 0], gy_r.at[i - 1])
            landed(gathered.at[:, source, near], gh_r.at[Z_FAR.index(Z_NEAR[i - 1])])

        def decode(group, _, source=source):
            for j in range(per):
                sums = eighth_root(gathered[group, source, j])
                gradient_ref[row_of(group), aligned(source * per + j)] = (
                    sums * spread[source * per + j, row_of(group)]
                )
            return 0

        lax.fori_loop(0, NY, decode, 0, unroll=2)

    load_momentum.wait()
    add_up(2, 10, 7, one_r.at[QC])
    square_total = jnp.sum(squares[3], axis=(0, 1), keepdims=True)
    root_mean = jnp.sqrt(square_total / entry_count + epsilon)
    factor_ref[...] = jnp.broadcast_to(jnp.minimum(1.0, clip_level / root_mean), (8, BLOCK))

    for ref, n in (
        (maxima_y, MY), (maxima_z, MZ), (maxima_y.at[:, 0], MA), (raw_y, RY), (raw_z, RZ), (parts_z, PZ),
        (parts_y, PY), (parts_z, GZ), (raw_z.at[pl.ds(0, NY - 1)], GO),
        (raw_y.at[:, pl.ds(0, NZ - 1)], GY), (raw_z, GH), (squares_in.at[pl.ds(0, 7)], QC),
        (squares_in.at[pl.ds(7, 3)], QY), (squares_in.at[pl.ds(10, 7)], QZ),
    ):
        all_of(ref, one_s.at[n], one_r.at[n]).wait_send()


def outer_step(
    gradient_ref, factor_ref, scales_ref, outer_ref, momentum_ref,
    params_hbm, momentum_hbm, scales_hbm, params_v, momentum_v, sem,
):
    parts, part = params_v.shape[0], params_v.shape[1]
    copies = [pltpu.make_async_copy(scales_ref, scales_hbm, sem.at[2 * parts])]
    copies[0].start()
    factor = factor_ref[0:1, 0:1]
    for i in range(parts):
        where = pl.ds(i * part, part)
        clipped = factor * gradient_ref[where]
        after = outer_decay * momentum_ref[where] + clipped
        momentum_v[i] = after
        params_v[i] = outer_ref[where] - outer_rate * (clipped + outer_decay * after)
        for k, (src, dst) in enumerate(((params_v, params_hbm), (momentum_v, momentum_hbm))):
            copies.append(pltpu.make_async_copy(src.at[i], dst.at[where], sem.at[2 * i + k]))
            copies[-1].start()
    for c in copies:
        c.wait()


def per_device(outer_params, local_params, momentum):
    rows, cols = outer_params.shape
    nr, nc = rows // NY, cols // NZ
    vmem = pltpu.VMEM
    dma = pltpu.SemaphoreType.DMA
    outs = pl.pallas_call(
        kernel,
        out_shape=(
            jax.ShapeDtypeStruct((rows, cols), F32),
            jax.ShapeDtypeStruct((8, BLOCK), F32),
            jax.ShapeDtypeStruct((cols // BLOCK, rows), F32),
            jax.ShapeDtypeStruct((rows, cols), F32),
            jax.ShapeDtypeStruct((rows, cols), F32),
        ),
        in_specs=[pl.BlockSpec(memory_space=pltpu.HBM)] * 3,
        out_specs=[pl.BlockSpec(memory_space=pltpu.VMEM)] * 5,
        scratch_shapes=[
            vmem((rows, cols), BF16),
            vmem((NY + 1, 8, BLOCK), F32),
            vmem((NY - 1, 2, 8, BLOCK), F32),
            vmem((2, 8, BLOCK), F32),
            vmem((NZ - 1, 2, 8, BLOCK), F32),
            vmem((NY, 8, BLOCK), F32),
            vmem((cols // BLOCK, nr, BLOCK), F32),
            vmem((rows, BLOCK), F32),
            vmem((cols // BLOCK, rows, BLOCK), F32),
            vmem((NY - 1, NZ, nr, nc - BLOCK), BF16),
            vmem((NZ - 1, rows, BLOCK), BF16),
            vmem((NZ - 1, nr, nc - BLOCK), BF16),
            vmem((NY, nr, BLOCK), BF16),
            vmem((nr, nc), F32),
            vmem((NZ - 1, nr, nc - BLOCK), BF16),
            vmem((NY - 1, nr, BLOCK), BF16),
            vmem((NY, NZ, nc // BLOCK, nr, BLOCK), BF16),
            vmem((4, 8, BLOCK), F32),
            vmem((17, 8, BLOCK), F32),
            dma((3, NY)), dma((14,)), dma((14,)),
            dma((NZ,)), dma((NZ - 1,)), dma((NZ - 1,)), dma((NZ - 1,)),
        ],
        compiler_params=pltpu.CompilerParams(
            collective_id=0, has_side_effects=True, vmem_limit_bytes=32 * 1024 * 1024
        ),
        name="synchronise",
    )(*[pltpu.with_memory_space_constraint(a, pltpu.HBM) for a in (outer_params, local_params, momentum)])


    parts = 8
    return pl.pallas_call(
        outer_step,
        out_shape=[
            jax.ShapeDtypeStruct((rows, cols), F32),
            jax.ShapeDtypeStruct((rows, cols), F32),
            jax.ShapeDtypeStruct((cols // BLOCK, rows), F32),
        ],
        in_specs=[pl.BlockSpec(memory_space=pltpu.VMEM)] * 5,
        out_specs=[pl.BlockSpec(memory_space=pltpu.HBM)] * 3,
        scratch_shapes=[
            vmem((parts, rows // parts, cols), F32),
            vmem((parts, rows // parts, cols), F32),
            dma((2 * parts + 1,)),
        ],
        compiler_params=pltpu.CompilerParams(vmem_limit_bytes=8 * 1024 * 1024),
        name="outer_step",
    )(*outs)


def solution(mesh):
    finer = Mesh(mesh.devices.reshape([SIZES[a] for a in AXES]), AXES)
    placed = (P(SHARD, None), P(REPLICA, SHARD, None), P(SHARD, None))
    return jax.shard_map(
        per_device,
        mesh=finer,
        in_specs=placed,
        out_specs=(P(SHARD, None), P(SHARD, None), P(None, SHARD)),
        check_vma=False,
    )
```

```python
import jax
import jax.numpy as jnp
from jax import lax
from jax.experimental import pallas as pl
from jax.experimental.pallas import tpu as pltpu
from jax.sharding import Mesh
from jax.sharding import PartitionSpec as P

F32, BF16 = jnp.float32, jnp.bfloat16
MESH = pl.DeviceIdType.MESH
BLOCK = 128
AXES = ("y", "z", "x", "core")
SIZES = {"y": 4, "z": 8, "x": 4, "core": 2}
REPLICA = ("y", "z")
SHARD = ("x", "core")
NY, NZ = SIZES["y"], SIZES["z"]
WORKERS = NY * NZ

epsilon = 1e-06
clip_level = 0.5
outer_rate = 0.7
outer_decay = 0.9
grid_levels = 7.0

CURVE = (
    6.579723256002266,
    -12.987145762286145,
    12.194590761626122,
    -6.583999071997054,
    1.9907873039801487,
)

Y_STEPS = (2, 1, 3)
Z_FAR = (4, 3, 5, 2, 6, 1, 7)
Z_NEAR = (1, 7, 2, 6, 3, 5, 4)
CELL = tuple((a, b) for a in range(4) for b in range(2) if (a, b) != (0, 0))


def curve(r):
    t = r * r
    p = CURVE[-1]
    for c in CURVE[-2::-1]:
        p = p * t + c
    return (r * t) * p


def smooth_round(v):
    whole = jnp.round(v)
    return whole + curve(curve(v - whole))


def eighth_power(s):
    t = s * s
    return (s * jnp.abs(s)) * t * (t * t)


def eighth_root(c):
    c = c.astype(F32)
    size = jnp.exp2(0.125 * jnp.log2(jnp.maximum(jnp.abs(c), 1e-37)))
    return jnp.where(c < 0.0, -size, size)


def kernel(
    outer_hbm, local_hbm, momentum_hbm, gradient_ref, factor_ref, scales_ref, outer_v, momentum_v,
    local_v, maxima, maxima_y, max_own, maxima_z, max_all,
    inverse, inverse_z, spread, raw_y, raw_z, partial, partial_y, total, parts_z, parts_y, gathered,
    squares, squares_in, load_sem, one_s, one_r, raw_r, gz_r, gy_r, gh_r,
):
    y, z = lax.axis_index("y"), lax.axis_index("z")
    x, core = lax.axis_index("x"), lax.axis_index("core")
    at = {"y": y, "z": z, "x": x, "core": core}
    rows, cols = outer_v.shape
    nr, nc = rows // NY, cols // NZ
    per = nc // BLOCK
    near = per - 1
    nb = cols // BLOCK
    entry_count = rows * cols * SIZES["x"] * SIZES["core"]
    lane = lax.broadcasted_iota(jnp.int32, (8, BLOCK), 1)
    MY, MZ, MA, RY, RZ, PZ, PY, GZ, GO, GY, GH, QC, QY, QZ = range(14)

    def peer(**steps):
        return {k: lax.rem(at[k] + s, SIZES[k]) for k, s in steps.items()}

    def send(src, dst, ss, rs, **steps):
        pltpu.make_async_remote_copy(
            src_ref=src, dst_ref=dst, send_sem=ss, recv_sem=rs,
            device_id=peer(**steps), device_id_type=MESH,
        ).start()

    def all_of(ref, ss, rs):
        return pltpu.make_async_remote_copy(
            src_ref=ref, dst_ref=ref, send_sem=ss, recv_sem=rs,
            device_id=peer(y=1), device_id_type=MESH,
        )

    def landed(ref, sem):
        all_of(ref, one_s.at[0], sem).wait_recv()

    def row_of(g):
        return pl.ds(pl.multiple_of(g * nr, nr), nr)

    def aligned(n, count=1):
        return pl.ds(pl.multiple_of(n * BLOCK, BLOCK), count * BLOCK)

    barrier = pltpu.get_barrier_semaphore()
    friends = (
        [dict(y=s) for s in range(1, NY)]
        + [dict(z=s) for s in range(1, NZ)]
        + [dict(x=a, core=b) for a, b in CELL]
    )
    for f in friends:
        pl.semaphore_signal(barrier, inc=1, device_id=peer(**f), device_id_type=MESH)

    load_momentum = pltpu.make_async_copy(momentum_hbm, momentum_v, load_sem.at[2, 0])
    loads = [
        pltpu.make_async_copy(src.at[pl.ds(g * nr, nr)], dst.at[pl.ds(g * nr, nr)], load_sem.at[k, g])
        for g in range(NY)
        for k, (src, dst) in enumerate(((local_hbm.at[0], local_v), (outer_hbm, outer_v)))
    ]
    for c in loads:
        c.start()

    lasts = jnp.zeros((8, BLOCK), F32)
    for g in range(NY):
        loads[2 * g].wait()
        loads[2 * g + 1].wait()

        def block_max(p, acc, g=g):
            out, lasts = acc
            for j in range(per):
                for r in range(nr // 8):
                    where = (pl.ds(g * nr + r * 8, 8), aligned(p * per + j))
                    deltas = outer_v[where] - local_v[where].astype(F32)
                    most = jnp.max(jnp.abs(deltas), axis=1, keepdims=True)
                    out = jnp.where(lane == r * nb + p * per + j, most, out)
                    if j == near:
                        lasts = jnp.where(lane == p * (rows // 8) + g * (nr // 8) + r, most, lasts)
            return out, lasts

        maxima[g], lasts = lax.fori_loop(
            0, NZ, block_max, (jnp.zeros((8, BLOCK), F32), lasts), unroll=4
        )
    maxima[NY] = lasts

    load_momentum.start()
    pl.semaphore_wait(barrier, len(friends))

    order = (4, 3, 5, 2, 6, 1, 7, 0)
    pieces = [lax.rem(z + o, NZ) for o in order]

    def send_raw_y(i):
        for k, s in enumerate(Y_STEPS):
            send(
                local_v.at[row_of(lax.rem(y + s, NY)), aligned(pieces[i] * per, near)],
                raw_y.at[k, i], one_s.at[RY], raw_r.at[i], y=s,
            )

    def send_raw_z(i):
        s = Z_FAR[i]
        send(
            local_v.at[:, aligned(lax.rem(z + s, NZ) * per + near)],
            raw_z.at[i], one_s.at[RZ], one_r.at[RZ], z=s,
        )

    for i, s in enumerate(Y_STEPS):
        send(maxima.at[lax.rem(y + s, NY)], maxima_y.at[i, 0], one_s.at[MY], one_r.at[MY], y=s)
        send(maxima.at[NY], maxima_y.at[i, 1], one_s.at[MY], one_r.at[MY], y=s)
    for i in range(NZ):
        send_raw_y(i)
        if i < 3:
            send_raw_z(i)
    landed(maxima_y, one_r.at[MY])
    for k, row in enumerate((y, NY)):
        m = maxima[row]
        for i in range(len(Y_STEPS)):
            m = jnp.maximum(m, maxima_y[i, k])
        max_own[k] = m
    for i, s in enumerate(Z_FAR):
        send(max_own, maxima_z.at[i], one_s.at[MZ], one_r.at[MZ], z=s)
    for i in range(3, NZ - 1):
        send_raw_z(i)
    landed(maxima_z, one_r.at[MZ])
    m, lasts = max_own[0], max_own[1]
    for i in range(len(Z_FAR)):
        m = jnp.maximum(m, maxima_z[i, 0])
        lasts = jnp.maximum(lasts, maxima_z[i, 1])
    max_all[y] = m
    for s in Y_STEPS:
        send(max_all.at[y], max_all.at[y], one_s.at[MA], one_r.at[MA], y=s)

    inverse_scale = grid_levels / (m + epsilon)
    for b in range(nb):
        for r in range(nr // 8):
            n = r * nb + b
            inverse[b, pl.ds(r * 8, 8), :] = jnp.broadcast_to(
                inverse_scale[:, n : n + 1], (8, BLOCK)
            )

    def encoded(o, local, inv):
        v = (o - local.astype(F32)) * inv
        return smooth_round(v).astype(BF16).astype(F32)

    def along_y(i):
        p = pieces[i]
        landed(raw_y.at[:, i], raw_r.at[i])

        def encode(j, _):
            lanes = aligned(j)
            columns = aligned(p * per + j)
            o = outer_v[row_of(y), columns]
            inv = inverse[p * per + j]
            acc = encoded(o, local_v[row_of(y), columns], inv)
            for k in range(len(Y_STEPS)):
                acc += encoded(o, raw_y[k, i, :, lanes], inv)
            if i < NZ - 1:
                partial[i, :, lanes] = eighth_power(acc).astype(BF16)
            else:
                total[:, lanes] = acc
            return 0

        lax.fori_loop(0, near, encode, 0, unroll=True)
        if i < NZ - 1:
            send(partial.at[i], parts_z.at[i], one_s.at[PZ], one_r.at[PZ], z=order[i])

    def along_z():
        landed(raw_z, one_r.at[RZ])
        last = z * per + near
        turned = pltpu.roll(grid_levels / (lasts + epsilon), BLOCK - z * (rows // 8), 1)
        for r in range(rows // 8):
            inverse_z[pl.ds(r * 8, 8), :] = jnp.broadcast_to(turned[:, r : r + 1], (8, BLOCK))

        def encode(g, _):
            inv = inverse_z[row_of(g), :]
            o = outer_v[row_of(g), aligned(last)]
            acc = encoded(o, local_v[row_of(g), aligned(last)], inv)
            for k in range(NZ - 1):
                acc += encoded(o, raw_z[k, row_of(g), :], inv)
            partial_y[g] = eighth_power(acc).astype(BF16)

            @pl.when(g == y)
            def _():
                total[:, pl.ds(near * BLOCK, BLOCK)] = acc

            return 0

        lax.fori_loop(0, NY, encode, 0, unroll=2)
        for k, s in enumerate(Y_STEPS):
            send(partial_y.at[lax.rem(y + s, NY)], parts_y.at[k], one_s.at[PY], one_r.at[PY], y=s)

    for i in range(5):
        along_y(i)
    along_z()
    for i in range(5, NZ):
        along_y(i)
    landed(maxima_y.at[:, 0], one_r.at[MA])
    def spread_scale(g):
        group_scale = (max_all[g] + epsilon) * (1.0 / (grid_levels * WORKERS))
        for b in range(nb):
            for r in range(nr // 8):
                n = r * nb + b
                spread[b, pl.ds(g * nr + r * 8, 8), :] = jnp.broadcast_to(
                    group_scale[:, n : n + 1], (8, BLOCK)
                )

    for g in range(NY):
        spread_scale(g)

    stack = []
    for g in range(NY):
        for r in range(nr // 8):
            turned = max_all[g] if r == 0 else pltpu.roll(max_all[g], BLOCK - r * nb, 1)
            stack.append(turned)
    scales_ref[...] = jnp.concatenate(stack, axis=0).T[:nb]

    landed(parts_z, one_r.at[PZ])
    landed(parts_y, one_r.at[PY])

    sq = jnp.zeros((8, BLOCK), F32)
    for j in range(per):
        lanes = pl.ds(j * BLOCK, BLOCK)
        acc = total[:, lanes]
        if j < near:
            for i in range(NZ - 1):
                acc += eighth_root(parts_z[i, :, lanes])
        else:
            for i in range(NY - 1):
                acc += eighth_root(parts_y[i])
        gathered[y, z, j] = eighth_power(acc).astype(BF16)
        g = acc / inverse[z * per + j] * (1.0 / WORKERS)
        g2 = g * g
        for r in range(nr // 8):
            sq += g2[r * 8 : r * 8 + 8]
    squares[0] = sq

    most = pl.ds(0, near)

    def pass_on(i):
        source = lax.rem(z + NZ - Z_NEAR[i], NZ)
        ref = gathered.at[y, source, most]
        landed(ref, gz_r.at[i])
        for s in Y_STEPS:
            send(ref, ref, one_s.at[GY], gy_r.at[i], y=s)

    def pass_last(i):
        ref = gathered.at[:, z, near]
        send(ref, ref, one_s.at[GH], gh_r.at[i], z=Z_FAR[i])

    def add_up(slot, first, count, sem):
        landed(squares_in.at[pl.ds(first, count)], sem)
        acc = squares[slot]
        for i in range(count):
            acc += squares_in[first + i]
        squares[slot + 1] = acc

    for i, s in enumerate(Z_NEAR):
        send(squares.at[0], squares_in.at[i], one_s.at[QZ], one_r.at[QZ], z=s)
    ref = gathered.at[y, z, most]
    for i, s in enumerate(Z_NEAR):
        send(ref, ref, one_s.at[GZ], gz_r.at[i], z=s)
    ref = gathered.at[y, z]
    for s in Y_STEPS:
        send(ref, ref, one_s.at[GO], one_r.at[GO], y=s)

    pass_on(0)
    pass_on(1)
    landed(raw_z.at[pl.ds(0, NY - 1)], one_r.at[GO])
    for i in range(NZ - 1):
        pass_last(i)
    add_up(0, 0, 7, one_r.at[QZ])
    for i, s in enumerate(Y_STEPS):
        send(squares.at[1], squares_in.at[7 + i], one_s.at[QY], one_r.at[QY], y=s)
    pass_on(2)
    pass_on(3)
    pass_on(4)
    pass_on(5)
    pass_on(6)
    add_up(1, 7, 3, one_r.at[QY])
    for i, (a, b) in enumerate(CELL):
        send(squares.at[2], squares_in.at[10 + i], one_s.at[QC], one_r.at[QC], x=a, core=b)

    for i in range(NZ):
        source = z if i == 0 else lax.rem(z + NZ - Z_NEAR[i - 1], NZ)
        if i > 0:
            landed(raw_y.at[:, 0], gy_r.at[i - 1])
            landed(gathered.at[:, source, near], gh_r.at[Z_FAR.index(Z_NEAR[i - 1])])

        def decode(group, _, source=source):
            for j in range(per):
                sums = eighth_root(gathered[group, source, j])
                gradient_ref[row_of(group), aligned(source * per + j)] = (
                    sums * spread[source * per + j, row_of(group)]
                )
            return 0

        lax.fori_loop(0, NY, decode, 0, unroll=True)

    load_momentum.wait()
    add_up(2, 10, 7, one_r.at[QC])
    square_total = jnp.sum(squares[3], axis=(0, 1), keepdims=True)
    root_mean = jnp.sqrt(square_total / entry_count + epsilon)
    factor_ref[...] = jnp.broadcast_to(jnp.minimum(1.0, clip_level / root_mean), (8, BLOCK))

    for ref, n in (
        (maxima_y, MY), (maxima_z, MZ), (maxima_y.at[:, 0], MA), (raw_y, RY), (raw_z, RZ), (parts_z, PZ),
        (parts_y, PY), (parts_z, GZ), (raw_z.at[pl.ds(0, NY - 1)], GO),
        (raw_y.at[:, pl.ds(0, NZ - 1)], GY), (raw_z, GH), (squares_in.at[pl.ds(0, 7)], QC),
        (squares_in.at[pl.ds(7, 3)], QY), (squares_in.at[pl.ds(10, 7)], QZ),
    ):
        all_of(ref, one_s.at[n], one_r.at[n]).wait_send()


def outer_step(
    gradient_ref, factor_ref, scales_ref, outer_ref, momentum_ref,
    params_hbm, momentum_hbm, scales_hbm, params_v, momentum_v, sem,
):
    parts, part = params_v.shape[0], params_v.shape[1]
    copies = [pltpu.make_async_copy(scales_ref, scales_hbm, sem.at[2 * parts])]
    copies[0].start()
    factor = factor_ref[0:1, 0:1]
    for i in range(parts):
        where = pl.ds(i * part, part)
        clipped = factor * gradient_ref[where]
        after = outer_decay * momentum_ref[where] + clipped
        momentum_v[i] = after
        params_v[i] = outer_ref[where] - outer_rate * (clipped + outer_decay * after)
        for k, (src, dst) in enumerate(((params_v, params_hbm), (momentum_v, momentum_hbm))):
            copies.append(pltpu.make_async_copy(src.at[i], dst.at[where], sem.at[2 * i + k]))
            copies[-1].start()
    for c in copies:
        c.wait()


def per_device(outer_params, local_params, momentum):
    rows, cols = outer_params.shape
    nr, nc = rows // NY, cols // NZ
    vmem = pltpu.VMEM
    dma = pltpu.SemaphoreType.DMA
    outs = pl.pallas_call(
        kernel,
        out_shape=(
            jax.ShapeDtypeStruct((rows, cols), F32),
            jax.ShapeDtypeStruct((8, BLOCK), F32),
            jax.ShapeDtypeStruct((cols // BLOCK, rows), F32),
            jax.ShapeDtypeStruct((rows, cols), F32),
            jax.ShapeDtypeStruct((rows, cols), F32),
        ),
        in_specs=[pl.BlockSpec(memory_space=pltpu.HBM)] * 3,
        out_specs=[pl.BlockSpec(memory_space=pltpu.VMEM)] * 5,
        scratch_shapes=[
            vmem((rows, cols), BF16),
            vmem((NY + 1, 8, BLOCK), F32),
            vmem((NY - 1, 2, 8, BLOCK), F32),
            vmem((2, 8, BLOCK), F32),
            vmem((NZ - 1, 2, 8, BLOCK), F32),
            vmem((NY, 8, BLOCK), F32),
            vmem((cols // BLOCK, nr, BLOCK), F32),
            vmem((rows, BLOCK), F32),
            vmem((cols // BLOCK, rows, BLOCK), F32),
            vmem((NY - 1, NZ, nr, nc - BLOCK), BF16),
            vmem((NZ - 1, rows, BLOCK), BF16),
            vmem((NZ - 1, nr, nc - BLOCK), BF16),
            vmem((NY, nr, BLOCK), BF16),
            vmem((nr, nc), F32),
            vmem((NZ - 1, nr, nc - BLOCK), BF16),
            vmem((NY - 1, nr, BLOCK), BF16),
            vmem((NY, NZ, nc // BLOCK, nr, BLOCK), BF16),
            vmem((4, 8, BLOCK), F32),
            vmem((17, 8, BLOCK), F32),
            dma((3, NY)), dma((14,)), dma((14,)),
            dma((NZ,)), dma((NZ - 1,)), dma((NZ - 1,)), dma((NZ - 1,)),
        ],
        compiler_params=pltpu.CompilerParams(
            collective_id=0, has_side_effects=True, vmem_limit_bytes=32 * 1024 * 1024
        ),
        name="synchronise",
    )(*[pltpu.with_memory_space_constraint(a, pltpu.HBM) for a in (outer_params, local_params, momentum)])


    parts = 8
    return pl.pallas_call(
        outer_step,
        out_shape=[
            jax.ShapeDtypeStruct((rows, cols), F32),
            jax.ShapeDtypeStruct((rows, cols), F32),
            jax.ShapeDtypeStruct((cols // BLOCK, rows), F32),
        ],
        in_specs=[pl.BlockSpec(memory_space=pltpu.VMEM)] * 5,
        out_specs=[pl.BlockSpec(memory_space=pltpu.HBM)] * 3,
        scratch_shapes=[
            vmem((parts, rows // parts, cols), F32),
            vmem((parts, rows // parts, cols), F32),
            dma((2 * parts + 1,)),
        ],
        compiler_params=pltpu.CompilerParams(vmem_limit_bytes=8 * 1024 * 1024),
        name="outer_step",
    )(*outs)


def solution(mesh):
    finer = Mesh(mesh.devices.reshape([SIZES[a] for a in AXES]), AXES)
    placed = (P(SHARD, None), P(REPLICA, SHARD, None), P(SHARD, None))
    return jax.shard_map(
        per_device,
        mesh=finer,
        in_specs=placed,
        out_specs=(P(SHARD, None), P(SHARD, None), P(None, SHARD)),
        check_vma=False,
    )
```

```python
import jax
import jax.numpy as jnp
from jax import lax
from jax.experimental import pallas as pl
from jax.experimental.pallas import tpu as pltpu
from jax.sharding import Mesh
from jax.sharding import PartitionSpec as P

F32, BF16 = jnp.float32, jnp.bfloat16
MESH = pl.DeviceIdType.MESH
BLOCK = 128
AXES = ("y", "z", "x", "core")
SIZES = {"y": 4, "z": 8, "x": 4, "core": 2}
REPLICA = ("y", "z")
SHARD = ("x", "core")
NY, NZ = SIZES["y"], SIZES["z"]
WORKERS = NY * NZ

epsilon = 1e-06
clip_level = 0.5
outer_rate = 0.7
outer_decay = 0.9
grid_levels = 7.0

CURVE = (
    6.579723256002266,
    -12.987145762286145,
    12.194590761626122,
    -6.583999071997054,
    1.9907873039801487,
)

Y_STEPS = (2, 1, 3)
Z_FAR = (4, 3, 5, 2, 6, 1, 7)
Z_NEAR = (1, 7, 2, 6, 3, 5, 4)
CELL = tuple((a, b) for a in range(4) for b in range(2) if (a, b) != (0, 0))


def curve(r):
    t = r * r
    p = CURVE[-1]
    for c in CURVE[-2::-1]:
        p = p * t + c
    return (r * t) * p


def smooth_round(v):
    whole = jnp.round(v)
    return whole + curve(curve(v - whole))


def eighth_power(s):
    t = s * s
    return (s * jnp.abs(s)) * t * (t * t)


def eighth_root(c):
    c = c.astype(F32)
    size = jnp.exp2(0.125 * jnp.log2(jnp.maximum(jnp.abs(c), 1e-37)))
    return jnp.where(c < 0.0, -size, size)


def kernel(
    outer_hbm, local_hbm, momentum_hbm, gradient_ref, factor_ref, scales_ref, outer_v, momentum_v,
    local_v, maxima, maxima_y, max_own, maxima_z, max_all,
    inverse, inverse_z, spread, raw_y, raw_z, partial, partial_y, total, parts_z, parts_y, gathered,
    squares, squares_in, load_sem, one_s, one_r, raw_r, gz_r, gy_r, gh_r,
):
    y, z = lax.axis_index("y"), lax.axis_index("z")
    x, core = lax.axis_index("x"), lax.axis_index("core")
    at = {"y": y, "z": z, "x": x, "core": core}
    rows, cols = outer_v.shape
    nr, nc = rows // NY, cols // NZ
    per = nc // BLOCK
    near = per - 1
    nb = cols // BLOCK
    entry_count = rows * cols * SIZES["x"] * SIZES["core"]
    lane = lax.broadcasted_iota(jnp.int32, (8, BLOCK), 1)
    MY, MZ, MA, RY, RZ, PZ, PY, GZ, GO, GY, GH, QC, QY, QZ = range(14)

    def peer(**steps):
        return {k: lax.rem(at[k] + s, SIZES[k]) for k, s in steps.items()}

    def send(src, dst, ss, rs, **steps):
        pltpu.make_async_remote_copy(
            src_ref=src, dst_ref=dst, send_sem=ss, recv_sem=rs,
            device_id=peer(**steps), device_id_type=MESH,
        ).start()

    def all_of(ref, ss, rs):
        return pltpu.make_async_remote_copy(
            src_ref=ref, dst_ref=ref, send_sem=ss, recv_sem=rs,
            device_id=peer(y=1), device_id_type=MESH,
        )

    def landed(ref, sem):
        all_of(ref, one_s.at[0], sem).wait_recv()

    def row_of(g):
        return pl.ds(pl.multiple_of(g * nr, nr), nr)

    def aligned(n, count=1):
        return pl.ds(pl.multiple_of(n * BLOCK, BLOCK), count * BLOCK)

    load_momentum = pltpu.make_async_copy(momentum_hbm, momentum_v, load_sem.at[2, 0])
    loads = [
        pltpu.make_async_copy(src.at[pl.ds(g * nr, nr)], dst.at[pl.ds(g * nr, nr)], load_sem.at[k, g])
        for g in range(NY)
        for k, (src, dst) in enumerate(((local_hbm.at[0], local_v), (outer_hbm, outer_v)))
    ]
    for c in loads:
        c.start()

    barrier = pltpu.get_barrier_semaphore()
    friends = (
        [dict(y=s) for s in range(1, NY)]
        + [dict(z=s) for s in range(1, NZ)]
        + [dict(x=a, core=b) for a, b in CELL]
    )
    for f in friends:
        pl.semaphore_signal(barrier, inc=1, device_id=peer(**f), device_id_type=MESH)

    lasts = jnp.zeros((8, BLOCK), F32)
    for g in range(NY):
        loads[2 * g].wait()
        loads[2 * g + 1].wait()

        def block_max(p, acc, g=g):
            out, lasts = acc
            for j in range(per):
                for r in range(nr // 8):
                    where = (pl.ds(g * nr + r * 8, 8), aligned(p * per + j))
                    deltas = outer_v[where] - local_v[where].astype(F32)
                    most = jnp.max(jnp.abs(deltas), axis=1, keepdims=True)
                    out = jnp.where(lane == r * nb + p * per + j, most, out)
                    if j == near:
                        lasts = jnp.where(lane == p * (rows // 8) + g * (nr // 8) + r, most, lasts)
            return out, lasts

        maxima[g], lasts = lax.fori_loop(
            0, NZ, block_max, (jnp.zeros((8, BLOCK), F32), lasts), unroll=4
        )
    maxima[NY] = lasts

    load_momentum.start()
    pl.semaphore_wait(barrier, len(friends))

    order = (4, 3, 5, 2, 6, 1, 7, 0)
    pieces = [lax.rem(z + o, NZ) for o in order]

    def send_raw_y(i):
        for k, s in enumerate(Y_STEPS):
            send(
                local_v.at[row_of(lax.rem(y + s, NY)), aligned(pieces[i] * per, near)],
                raw_y.at[k, i], one_s.at[RY], raw_r.at[i], y=s,
            )

    def send_raw_z(i):
        s = Z_FAR[i]
        send(
            local_v.at[:, aligned(lax.rem(z + s, NZ) * per + near)],
            raw_z.at[i], one_s.at[RZ], one_r.at[RZ], z=s,
        )

    for i, s in enumerate(Y_STEPS):
        send(maxima.at[lax.rem(y + s, NY)], maxima_y.at[i, 0], one_s.at[MY], one_r.at[MY], y=s)
        send(maxima.at[NY], maxima_y.at[i, 1], one_s.at[MY], one_r.at[MY], y=s)
    for i in range(NZ):
        send_raw_y(i)
        if i < 3:
            send_raw_z(i)
    landed(maxima_y, one_r.at[MY])
    for k, row in enumerate((y, NY)):
        m = maxima[row]
        for i in range(len(Y_STEPS)):
            m = jnp.maximum(m, maxima_y[i, k])
        max_own[k] = m
    for i, s in enumerate(Z_FAR):
        send(max_own, maxima_z.at[i], one_s.at[MZ], one_r.at[MZ], z=s)
    for i in range(3, NZ - 1):
        send_raw_z(i)
    landed(maxima_z, one_r.at[MZ])
    m, lasts = max_own[0], max_own[1]
    for i in range(len(Z_FAR)):
        m = jnp.maximum(m, maxima_z[i, 0])
        lasts = jnp.maximum(lasts, maxima_z[i, 1])
    max_all[y] = m
    for s in Y_STEPS:
        send(max_all.at[y], max_all.at[y], one_s.at[MA], one_r.at[MA], y=s)

    inverse_scale = grid_levels / (m + epsilon)
    for b in range(nb):
        for r in range(nr // 8):
            n = r * nb + b
            inverse[b, pl.ds(r * 8, 8), :] = jnp.broadcast_to(
                inverse_scale[:, n : n + 1], (8, BLOCK)
            )

    def encoded(o, local, inv):
        v = (o - local.astype(F32)) * inv
        return smooth_round(v).astype(BF16).astype(F32)

    def along_y(i):
        p = pieces[i]
        landed(raw_y.at[:, i], raw_r.at[i])

        def encode(j, _):
            lanes = aligned(j)
            columns = aligned(p * per + j)
            o = outer_v[row_of(y), columns]
            inv = inverse[p * per + j]
            acc = encoded(o, local_v[row_of(y), columns], inv)
            for k in range(len(Y_STEPS)):
                acc += encoded(o, raw_y[k, i, :, lanes], inv)
            if i < NZ - 1:
                partial[i, :, lanes] = eighth_power(acc).astype(BF16)
            else:
                total[:, lanes] = acc
            return 0

        lax.fori_loop(0, near, encode, 0, unroll=True)
        if i < NZ - 1:
            send(partial.at[i], parts_z.at[i], one_s.at[PZ], one_r.at[PZ], z=order[i])

    def along_z():
        landed(raw_z, one_r.at[RZ])
        last = z * per + near
        turned = pltpu.roll(grid_levels / (lasts + epsilon), BLOCK - z * (rows // 8), 1)
        for r in range(rows // 8):
            inverse_z[pl.ds(r * 8, 8), :] = jnp.broadcast_to(turned[:, r : r + 1], (8, BLOCK))

        def encode(g, _):
            inv = inverse_z[row_of(g), :]
            o = outer_v[row_of(g), aligned(last)]
            acc = encoded(o, local_v[row_of(g), aligned(last)], inv)
            for k in range(NZ - 1):
                acc += encoded(o, raw_z[k, row_of(g), :], inv)
            partial_y[g] = eighth_power(acc).astype(BF16)

            @pl.when(g == y)
            def _():
                total[:, pl.ds(near * BLOCK, BLOCK)] = acc

            return 0

        lax.fori_loop(0, NY, encode, 0, unroll=2)
        for k, s in enumerate(Y_STEPS):
            send(partial_y.at[lax.rem(y + s, NY)], parts_y.at[k], one_s.at[PY], one_r.at[PY], y=s)

    for i in range(5):
        along_y(i)
    along_z()
    for i in range(5, NZ):
        along_y(i)
    landed(maxima_y.at[:, 0], one_r.at[MA])
    def spread_scale(g):
        group_scale = (max_all[g] + epsilon) * (1.0 / (grid_levels * WORKERS))
        for b in range(nb):
            for r in range(nr // 8):
                n = r * nb + b
                spread[b, pl.ds(g * nr + r * 8, 8), :] = jnp.broadcast_to(
                    group_scale[:, n : n + 1], (8, BLOCK)
                )

    for g in range(NY):
        spread_scale(g)

    stack = []
    for g in range(NY):
        for r in range(nr // 8):
            turned = max_all[g] if r == 0 else pltpu.roll(max_all[g], BLOCK - r * nb, 1)
            stack.append(turned)
    scales_ref[...] = jnp.concatenate(stack, axis=0).T[:nb]

    landed(parts_z, one_r.at[PZ])
    landed(parts_y, one_r.at[PY])

    sq = jnp.zeros((8, BLOCK), F32)
    for j in range(per):
        lanes = pl.ds(j * BLOCK, BLOCK)
        acc = total[:, lanes]
        if j < near:
            for i in range(NZ - 1):
                acc += eighth_root(parts_z[i, :, lanes])
        else:
            for i in range(NY - 1):
                acc += eighth_root(parts_y[i])
        gathered[y, z, j] = eighth_power(acc).astype(BF16)
        g = acc / inverse[z * per + j] * (1.0 / WORKERS)
        g2 = g * g
        for r in range(nr // 8):
            sq += g2[r * 8 : r * 8 + 8]
    squares[0] = sq

    most = pl.ds(0, near)

    def pass_on(i):
        source = lax.rem(z + NZ - Z_NEAR[i], NZ)
        ref = gathered.at[y, source, most]
        landed(ref, gz_r.at[i])
        for s in Y_STEPS:
            send(ref, ref, one_s.at[GY], gy_r.at[i], y=s)

    def pass_last(i):
        ref = gathered.at[:, z, near]
        send(ref, ref, one_s.at[GH], gh_r.at[i], z=Z_FAR[i])

    def add_up(slot, first, count, sem):
        landed(squares_in.at[pl.ds(first, count)], sem)
        acc = squares[slot]
        for i in range(count):
            acc += squares_in[first + i]
        squares[slot + 1] = acc

    for i, s in enumerate(Z_NEAR):
        send(squares.at[0], squares_in.at[i], one_s.at[QZ], one_r.at[QZ], z=s)
    ref = gathered.at[y, z, most]
    for i, s in enumerate(Z_NEAR):
        send(ref, ref, one_s.at[GZ], gz_r.at[i], z=s)
    ref = gathered.at[y, z]
    for s in Y_STEPS:
        send(ref, ref, one_s.at[GO], one_r.at[GO], y=s)

    pass_on(0)
    pass_on(1)
    landed(raw_z.at[pl.ds(0, NY - 1)], one_r.at[GO])
    for i in range(NZ - 1):
        pass_last(i)
    add_up(0, 0, 7, one_r.at[QZ])
    for i, s in enumerate(Y_STEPS):
        send(squares.at[1], squares_in.at[7 + i], one_s.at[QY], one_r.at[QY], y=s)
    pass_on(2)
    pass_on(3)
    pass_on(4)
    pass_on(5)
    pass_on(6)
    add_up(1, 7, 3, one_r.at[QY])
    for i, (a, b) in enumerate(CELL):
        send(squares.at[2], squares_in.at[10 + i], one_s.at[QC], one_r.at[QC], x=a, core=b)

    for i in range(NZ):
        source = z if i == 0 else lax.rem(z + NZ - Z_NEAR[i - 1], NZ)
        if i > 0:
            landed(raw_y.at[:, 0], gy_r.at[i - 1])
            landed(gathered.at[:, source, near], gh_r.at[Z_FAR.index(Z_NEAR[i - 1])])

        def decode(group, _, source=source):
            for j in range(per):
                sums = eighth_root(gathered[group, source, j])
                gradient_ref[row_of(group), aligned(source * per + j)] = (
                    sums * spread[source * per + j, row_of(group)]
                )
            return 0

        lax.fori_loop(0, NY, decode, 0, unroll=True)

    load_momentum.wait()
    add_up(2, 10, 7, one_r.at[QC])
    square_total = jnp.sum(squares[3], axis=(0, 1), keepdims=True)
    root_mean = jnp.sqrt(square_total / entry_count + epsilon)
    factor_ref[...] = jnp.broadcast_to(jnp.minimum(1.0, clip_level / root_mean), (8, BLOCK))

    for ref, n in (
        (maxima_y, MY), (maxima_z, MZ), (maxima_y.at[:, 0], MA), (raw_y, RY), (raw_z, RZ), (parts_z, PZ),
        (parts_y, PY), (parts_z, GZ), (raw_z.at[pl.ds(0, NY - 1)], GO),
        (raw_y.at[:, pl.ds(0, NZ - 1)], GY), (raw_z, GH), (squares_in.at[pl.ds(0, 7)], QC),
        (squares_in.at[pl.ds(7, 3)], QY), (squares_in.at[pl.ds(10, 7)], QZ),
    ):
        all_of(ref, one_s.at[n], one_r.at[n]).wait_send()


def outer_step(
    gradient_ref, factor_ref, scales_ref, outer_ref, momentum_ref,
    params_hbm, momentum_hbm, scales_hbm, params_v, momentum_v, sem,
):
    parts, part = params_v.shape[0], params_v.shape[1]
    copies = [pltpu.make_async_copy(scales_ref, scales_hbm, sem.at[2 * parts])]
    copies[0].start()
    factor = factor_ref[0:1, 0:1]
    for i in range(parts):
        where = pl.ds(i * part, part)
        clipped = factor * gradient_ref[where]
        after = outer_decay * momentum_ref[where] + clipped
        momentum_v[i] = after
        params_v[i] = outer_ref[where] - outer_rate * (clipped + outer_decay * after)
        for k, (src, dst) in enumerate(((params_v, params_hbm), (momentum_v, momentum_hbm))):
            copies.append(pltpu.make_async_copy(src.at[i], dst.at[where], sem.at[2 * i + k]))
            copies[-1].start()
    for c in copies:
        c.wait()


def per_device(outer_params, local_params, momentum):
    rows, cols = outer_params.shape
    nr, nc = rows // NY, cols // NZ
    vmem = pltpu.VMEM
    dma = pltpu.SemaphoreType.DMA
    outs = pl.pallas_call(
        kernel,
        out_shape=(
            jax.ShapeDtypeStruct((rows, cols), F32),
            jax.ShapeDtypeStruct((8, BLOCK), F32),
            jax.ShapeDtypeStruct((cols // BLOCK, rows), F32),
            jax.ShapeDtypeStruct((rows, cols), F32),
            jax.ShapeDtypeStruct((rows, cols), F32),
        ),
        in_specs=[pl.BlockSpec(memory_space=pltpu.HBM)] * 3,
        out_specs=[pl.BlockSpec(memory_space=pltpu.VMEM)] * 5,
        scratch_shapes=[
            vmem((rows, cols), BF16),
            vmem((NY + 1, 8, BLOCK), F32),
            vmem((NY - 1, 2, 8, BLOCK), F32),
            vmem((2, 8, BLOCK), F32),
            vmem((NZ - 1, 2, 8, BLOCK), F32),
            vmem((NY, 8, BLOCK), F32),
            vmem((cols // BLOCK, nr, BLOCK), F32),
            vmem((rows, BLOCK), F32),
            vmem((cols // BLOCK, rows, BLOCK), F32),
            vmem((NY - 1, NZ, nr, nc - BLOCK), BF16),
            vmem((NZ - 1, rows, BLOCK), BF16),
            vmem((NZ - 1, nr, nc - BLOCK), BF16),
            vmem((NY, nr, BLOCK), BF16),
            vmem((nr, nc), F32),
            vmem((NZ - 1, nr, nc - BLOCK), BF16),
            vmem((NY - 1, nr, BLOCK), BF16),
            vmem((NY, NZ, nc // BLOCK, nr, BLOCK), BF16),
            vmem((4, 8, BLOCK), F32),
            vmem((17, 8, BLOCK), F32),
            dma((3, NY)), dma((14,)), dma((14,)),
            dma((NZ,)), dma((NZ - 1,)), dma((NZ - 1,)), dma((NZ - 1,)),
        ],
        compiler_params=pltpu.CompilerParams(
            collective_id=0, has_side_effects=True, vmem_limit_bytes=32 * 1024 * 1024
        ),
        name="synchronise",
    )(*[pltpu.with_memory_space_constraint(a, pltpu.HBM) for a in (outer_params, local_params, momentum)])


    parts = 8
    return pl.pallas_call(
        outer_step,
        out_shape=[
            jax.ShapeDtypeStruct((rows, cols), F32),
            jax.ShapeDtypeStruct((rows, cols), F32),
            jax.ShapeDtypeStruct((cols // BLOCK, rows), F32),
        ],
        in_specs=[pl.BlockSpec(memory_space=pltpu.VMEM)] * 5,
        out_specs=[pl.BlockSpec(memory_space=pltpu.HBM)] * 3,
        scratch_shapes=[
            vmem((parts, rows // parts, cols), F32),
            vmem((parts, rows // parts, cols), F32),
            dma((2 * parts + 1,)),
        ],
        compiler_params=pltpu.CompilerParams(vmem_limit_bytes=8 * 1024 * 1024),
        name="outer_step",
    )(*outs)


def solution(mesh):
    finer = Mesh(mesh.devices.reshape([SIZES[a] for a in AXES]), AXES)
    placed = (P(SHARD, None), P(REPLICA, SHARD, None), P(SHARD, None))
    return jax.shard_map(
        per_device,
        mesh=finer,
        in_specs=placed,
        out_specs=(P(SHARD, None), P(SHARD, None), P(None, SHARD)),
        check_vma=False,
    )
```

```python
import jax
import jax.numpy as jnp
from jax import lax
from jax.experimental import pallas as pl
from jax.experimental.pallas import tpu as pltpu
from jax.sharding import Mesh
from jax.sharding import PartitionSpec as P

F32, BF16 = jnp.float32, jnp.bfloat16
MESH = pl.DeviceIdType.MESH
BLOCK = 128
AXES = ("y", "z", "x", "core")
SIZES = {"y": 4, "z": 8, "x": 4, "core": 2}
REPLICA = ("y", "z")
SHARD = ("x", "core")
NY, NZ = SIZES["y"], SIZES["z"]
WORKERS = NY * NZ

epsilon = 1e-06
clip_level = 0.5
outer_rate = 0.7
outer_decay = 0.9
grid_levels = 7.0

CURVE = (
    6.579723256002266,
    -12.987145762286145,
    12.194590761626122,
    -6.583999071997054,
    1.9907873039801487,
)

Y_STEPS = (2, 1, 3)
Z_FAR = (4, 3, 5, 2, 6, 1, 7)
Z_NEAR = (1, 7, 2, 6, 3, 5, 4)
CELL = tuple((a, b) for a in range(4) for b in range(2) if (a, b) != (0, 0))


def curve(r):
    t = r * r
    p = CURVE[-1]
    for c in CURVE[-2::-1]:
        p = p * t + c
    return (r * t) * p


def smooth_round(v):
    whole = jnp.round(v)
    return whole + curve(curve(v - whole))


def eighth_power(s):
    t = s * s
    return (s * jnp.abs(s)) * t * (t * t)


def eighth_root(c):
    c = c.astype(F32)
    size = jnp.exp2(0.125 * jnp.log2(jnp.maximum(jnp.abs(c), 1e-37)))
    return jnp.where(c < 0.0, -size, size)


def kernel(
    outer_hbm, local_hbm, momentum_hbm, gradient_ref, factor_ref, scales_ref, outer_v, momentum_v,
    local_v, maxima, maxima_y, max_own, maxima_z, max_all,
    inverse, inverse_z, spread, raw_y, raw_z, partial, partial_y, total, parts_z, parts_y, gathered,
    squares, squares_in, load_sem, one_s, one_r, raw_r, gz_r, gy_r, gh_r,
):
    y, z = lax.axis_index("y"), lax.axis_index("z")
    x, core = lax.axis_index("x"), lax.axis_index("core")
    at = {"y": y, "z": z, "x": x, "core": core}
    rows, cols = outer_v.shape
    nr, nc = rows // NY, cols // NZ
    per = nc // BLOCK
    near = per - 1
    nb = cols // BLOCK
    entry_count = rows * cols * SIZES["x"] * SIZES["core"]
    lane = lax.broadcasted_iota(jnp.int32, (8, BLOCK), 1)
    MY, MZ, MA, RY, RZ, PZ, PY, GZ, GO, GY, GH, QC, QY, QZ = range(14)

    def peer(**steps):
        return {k: lax.rem(at[k] + s, SIZES[k]) for k, s in steps.items()}

    def send(src, dst, ss, rs, **steps):
        pltpu.make_async_remote_copy(
            src_ref=src, dst_ref=dst, send_sem=ss, recv_sem=rs,
            device_id=peer(**steps), device_id_type=MESH,
        ).start()

    def all_of(ref, ss, rs):
        return pltpu.make_async_remote_copy(
            src_ref=ref, dst_ref=ref, send_sem=ss, recv_sem=rs,
            device_id=peer(y=1), device_id_type=MESH,
        )

    def landed(ref, sem):
        all_of(ref, one_s.at[0], sem).wait_recv()

    def row_of(g):
        return pl.ds(pl.multiple_of(g * nr, nr), nr)

    def aligned(n, count=1):
        return pl.ds(pl.multiple_of(n * BLOCK, BLOCK), count * BLOCK)

    load_momentum = pltpu.make_async_copy(momentum_hbm, momentum_v, load_sem.at[2, 0])
    loads = [
        pltpu.make_async_copy(src.at[pl.ds(g * nr, nr)], dst.at[pl.ds(g * nr, nr)], load_sem.at[k, g])
        for g in range(NY)
        for k, (src, dst) in enumerate(((local_hbm.at[0], local_v), (outer_hbm, outer_v)))
    ]
    for c in loads:
        c.start()

    barrier = pltpu.get_barrier_semaphore()
    friends = (
        [dict(y=s) for s in range(1, NY)]
        + [dict(z=s) for s in range(1, NZ)]
        + [dict(y=a, z=b) for a in range(1, NY) for b in (1, NZ - 1)]
        + [dict(x=a, core=b) for a, b in CELL]
    )
    for f in friends:
        pl.semaphore_signal(barrier, inc=1, device_id=peer(**f), device_id_type=MESH)

    lasts = jnp.zeros((8, BLOCK), F32)
    for g in range(NY):
        loads[2 * g].wait()
        loads[2 * g + 1].wait()

        def block_max(p, acc, g=g):
            out, lasts = acc
            for j in range(per):
                for r in range(nr // 8):
                    where = (pl.ds(g * nr + r * 8, 8), aligned(p * per + j))
                    deltas = outer_v[where] - local_v[where].astype(F32)
                    most = jnp.max(jnp.abs(deltas), axis=1, keepdims=True)
                    out = jnp.where(lane == r * nb + p * per + j, most, out)
                    if j == near:
                        lasts = jnp.where(lane == p * (rows // 8) + g * (nr // 8) + r, most, lasts)
            return out, lasts

        maxima[g], lasts = lax.fori_loop(
            0, NZ, block_max, (jnp.zeros((8, BLOCK), F32), lasts), unroll=4
        )
    maxima[NY] = lasts

    load_momentum.start()
    pl.semaphore_wait(barrier, len(friends))

    order = (4, 3, 5, 2, 6, 1, 7, 0)
    pieces = [lax.rem(z + o, NZ) for o in order]

    def send_raw_y(i):
        for k, s in enumerate(Y_STEPS):
            send(
                local_v.at[row_of(lax.rem(y + s, NY)), aligned(pieces[i] * per, near)],
                raw_y.at[k, i], one_s.at[RY], raw_r.at[i], y=s,
            )

    def send_raw_z(i):
        s = Z_FAR[i]
        send(
            local_v.at[:, aligned(lax.rem(z + s, NZ) * per + near)],
            raw_z.at[i], one_s.at[RZ], one_r.at[RZ], z=s,
        )

    for i, s in enumerate(Y_STEPS):
        send(maxima.at[lax.rem(y + s, NY)], maxima_y.at[i, 0], one_s.at[MY], one_r.at[MY], y=s)
        send(maxima.at[NY], maxima_y.at[i, 1], one_s.at[MY], one_r.at[MY], y=s)
    for i in range(NZ):
        send_raw_y(i)
        if i < 3:
            send_raw_z(i)
    landed(maxima_y, one_r.at[MY])
    for k, row in enumerate((y, NY)):
        m = maxima[row]
        for i in range(len(Y_STEPS)):
            m = jnp.maximum(m, maxima_y[i, k])
        max_own[k] = m
    for i, s in enumerate(Z_FAR):
        send(max_own, maxima_z.at[i], one_s.at[MZ], one_r.at[MZ], z=s)
    for i in range(3, NZ - 1):
        send_raw_z(i)
    landed(maxima_z, one_r.at[MZ])
    m, lasts = max_own[0], max_own[1]
    for i in range(len(Z_FAR)):
        m = jnp.maximum(m, maxima_z[i, 0])
        lasts = jnp.maximum(lasts, maxima_z[i, 1])
    max_all[y] = m
    for s in Y_STEPS:
        send(max_all.at[y], max_all.at[y], one_s.at[MA], one_r.at[MA], y=s)

    inverse_scale = grid_levels / (m + epsilon)
    for b in range(nb):
        for r in range(nr // 8):
            n = r * nb + b
            inverse[b, pl.ds(r * 8, 8), :] = jnp.broadcast_to(
                inverse_scale[:, n : n + 1], (8, BLOCK)
            )

    def encoded(o, local, inv):
        v = (o - local.astype(F32)) * inv
        return smooth_round(v).astype(BF16).astype(F32)

    def along_y(i):
        p = pieces[i]
        landed(raw_y.at[:, i], raw_r.at[i])

        def encode(j, _):
            lanes = aligned(j)
            columns = aligned(p * per + j)
            o = outer_v[row_of(y), columns]
            inv = inverse[p * per + j]
            acc = encoded(o, local_v[row_of(y), columns], inv)
            for k in range(len(Y_STEPS)):
                acc += encoded(o, raw_y[k, i, :, lanes], inv)
            if i < NZ - 1:
                partial[i, :, lanes] = eighth_power(acc).astype(BF16)
            else:
                total[:, lanes] = acc
            return 0

        lax.fori_loop(0, near, encode, 0, unroll=True)
        if i < NZ - 1:
            send(partial.at[i], parts_z.at[i], one_s.at[PZ], one_r.at[PZ], z=order[i])

    def along_z():
        landed(raw_z, one_r.at[RZ])
        last = z * per + near
        turned = pltpu.roll(grid_levels / (lasts + epsilon), BLOCK - z * (rows // 8), 1)
        for r in range(rows // 8):
            inverse_z[pl.ds(r * 8, 8), :] = jnp.broadcast_to(turned[:, r : r + 1], (8, BLOCK))

        def encode(g, _):
            inv = inverse_z[row_of(g), :]
            o = outer_v[row_of(g), aligned(last)]
            acc = encoded(o, local_v[row_of(g), aligned(last)], inv)
            for k in range(NZ - 1):
                acc += encoded(o, raw_z[k, row_of(g), :], inv)
            partial_y[g] = eighth_power(acc).astype(BF16)

            @pl.when(g == y)
            def _():
                total[:, pl.ds(near * BLOCK, BLOCK)] = acc

            return 0

        lax.fori_loop(0, NY, encode, 0, unroll=2)
        for k, s in enumerate(Y_STEPS):
            send(partial_y.at[lax.rem(y + s, NY)], parts_y.at[k], one_s.at[PY], one_r.at[PY], y=s)

    for i in range(5):
        along_y(i)
    along_z()
    for i in range(5, NZ):
        along_y(i)
    landed(maxima_y.at[:, 0], one_r.at[MA])
    def spread_scale(g):
        group_scale = (max_all[g] + epsilon) * (1.0 / (grid_levels * WORKERS))
        for b in range(nb):
            for r in range(nr // 8):
                n = r * nb + b
                spread[b, pl.ds(g * nr + r * 8, 8), :] = jnp.broadcast_to(
                    group_scale[:, n : n + 1], (8, BLOCK)
                )

    for g in range(NY):
        spread_scale(g)

    stack = []
    for g in range(NY):
        for r in range(nr // 8):
            turned = max_all[g] if r == 0 else pltpu.roll(max_all[g], BLOCK - r * nb, 1)
            stack.append(turned)
    scales_ref[...] = jnp.concatenate(stack, axis=0).T[:nb]

    landed(parts_z, one_r.at[PZ])
    landed(parts_y, one_r.at[PY])

    sq = jnp.zeros((8, BLOCK), F32)
    for j in range(per):
        lanes = pl.ds(j * BLOCK, BLOCK)
        acc = total[:, lanes]
        if j < near:
            for i in range(NZ - 1):
                acc += eighth_root(parts_z[i, :, lanes])
        else:
            for i in range(NY - 1):
                acc += eighth_root(parts_y[i])
        gathered[y, z, j] = eighth_power(acc).astype(BF16)
        g = acc / inverse[z * per + j] * (1.0 / WORKERS)
        g2 = g * g
        for r in range(nr // 8):
            sq += g2[r * 8 : r * 8 + 8]
    squares[0] = sq

    most = pl.ds(0, near)

    def pass_on(i):
        source = lax.rem(z + NZ - Z_NEAR[i], NZ)
        ref = gathered.at[y, source, most]
        landed(ref, gz_r.at[i])
        if i >= 2:
            for s in Y_STEPS:
                send(ref, ref, one_s.at[GY], gy_r.at[i], y=s)

    def pass_last(i):
        ref = gathered.at[:, z, near]
        send(ref, ref, one_s.at[GH], gh_r.at[i], z=Z_FAR[i])

    def add_up(slot, first, count, sem):
        landed(squares_in.at[pl.ds(first, count)], sem)
        acc = squares[slot]
        for i in range(count):
            acc += squares_in[first + i]
        squares[slot + 1] = acc

    for i, s in enumerate(Z_NEAR):
        send(squares.at[0], squares_in.at[i], one_s.at[QZ], one_r.at[QZ], z=s)
    ref = gathered.at[y, z, most]
    for i in reversed(range(2, NZ - 1)):
        send(ref, ref, one_s.at[GZ], gz_r.at[i], z=Z_NEAR[i])
    ref = gathered.at[y, z]
    for s in Y_STEPS:
        send(ref, ref, one_s.at[GO], one_r.at[GO], y=s)
    ref = gathered.at[y, z, most]
    for i in range(2):
        for s in Y_STEPS:
            send(ref, ref, one_s.at[GY], gy_r.at[i], y=s, z=Z_NEAR[i])
    for i in range(2):
        send(ref, ref, one_s.at[GZ], gz_r.at[i], z=Z_NEAR[i])

    landed(raw_z.at[pl.ds(0, NY - 1)], one_r.at[GO])
    for i in range(NZ - 1):
        pass_last(i)
    add_up(0, 0, 7, one_r.at[QZ])
    for i, s in enumerate(Y_STEPS):
        send(squares.at[1], squares_in.at[7 + i], one_s.at[QY], one_r.at[QY], y=s)
    pass_on(2)
    pass_on(3)
    pass_on(4)
    pass_on(5)
    pass_on(6)
    add_up(1, 7, 3, one_r.at[QY])
    for i, (a, b) in enumerate(CELL):
        send(squares.at[2], squares_in.at[10 + i], one_s.at[QC], one_r.at[QC], x=a, core=b)

    pass_on(0)
    pass_on(1)

    for i in range(NZ):
        source = z if i == 0 else lax.rem(z + NZ - Z_NEAR[i - 1], NZ)
        if i > 0:
            landed(raw_y.at[:, 0], gy_r.at[i - 1])
            landed(gathered.at[:, source, near], gh_r.at[Z_FAR.index(Z_NEAR[i - 1])])

        def decode(group, _, source=source):
            for j in range(per):
                sums = eighth_root(gathered[group, source, j])
                gradient_ref[row_of(group), aligned(source * per + j)] = (
                    sums * spread[source * per + j, row_of(group)]
                )
            return 0

        lax.fori_loop(0, NY, decode, 0, unroll=True)

    load_momentum.wait()
    add_up(2, 10, 7, one_r.at[QC])
    square_total = jnp.sum(squares[3], axis=(0, 1), keepdims=True)
    root_mean = jnp.sqrt(square_total / entry_count + epsilon)
    factor_ref[...] = jnp.broadcast_to(jnp.minimum(1.0, clip_level / root_mean), (8, BLOCK))

    for ref, n in (
        (maxima_y, MY), (maxima_z, MZ), (maxima_y.at[:, 0], MA), (raw_y, RY), (raw_z, RZ), (parts_z, PZ),
        (parts_y, PY), (parts_z, GZ), (raw_z.at[pl.ds(0, NY - 1)], GO),
        (raw_y.at[:, pl.ds(0, NZ - 1)], GY), (raw_z, GH), (squares_in.at[pl.ds(0, 7)], QC),
        (squares_in.at[pl.ds(7, 3)], QY), (squares_in.at[pl.ds(10, 7)], QZ),
    ):
        all_of(ref, one_s.at[n], one_r.at[n]).wait_send()


def outer_step(
    gradient_ref, factor_ref, scales_ref, outer_ref, momentum_ref,
    params_hbm, momentum_hbm, scales_hbm, params_v, momentum_v, sem,
):
    parts, part = params_v.shape[0], params_v.shape[1]
    copies = [pltpu.make_async_copy(scales_ref, scales_hbm, sem.at[2 * parts])]
    copies[0].start()
    factor = factor_ref[0:1, 0:1]
    for i in range(parts):
        where = pl.ds(i * part, part)
        clipped = factor * gradient_ref[where]
        after = outer_decay * momentum_ref[where] + clipped
        momentum_v[i] = after
        params_v[i] = outer_ref[where] - outer_rate * (clipped + outer_decay * after)
        for k, (src, dst) in enumerate(((params_v, params_hbm), (momentum_v, momentum_hbm))):
            copies.append(pltpu.make_async_copy(src.at[i], dst.at[where], sem.at[2 * i + k]))
            copies[-1].start()
    for c in copies:
        c.wait()


def per_device(outer_params, local_params, momentum):
    rows, cols = outer_params.shape
    nr, nc = rows // NY, cols // NZ
    vmem = pltpu.VMEM
    dma = pltpu.SemaphoreType.DMA
    outs = pl.pallas_call(
        kernel,
        out_shape=(
            jax.ShapeDtypeStruct((rows, cols), F32),
            jax.ShapeDtypeStruct((8, BLOCK), F32),
            jax.ShapeDtypeStruct((cols // BLOCK, rows), F32),
            jax.ShapeDtypeStruct((rows, cols), F32),
            jax.ShapeDtypeStruct((rows, cols), F32),
        ),
        in_specs=[pl.BlockSpec(memory_space=pltpu.HBM)] * 3,
        out_specs=[pl.BlockSpec(memory_space=pltpu.VMEM)] * 5,
        scratch_shapes=[
            vmem((rows, cols), BF16),
            vmem((NY + 1, 8, BLOCK), F32),
            vmem((NY - 1, 2, 8, BLOCK), F32),
            vmem((2, 8, BLOCK), F32),
            vmem((NZ - 1, 2, 8, BLOCK), F32),
            vmem((NY, 8, BLOCK), F32),
            vmem((cols // BLOCK, nr, BLOCK), F32),
            vmem((rows, BLOCK), F32),
            vmem((cols // BLOCK, rows, BLOCK), F32),
            vmem((NY - 1, NZ, nr, nc - BLOCK), BF16),
            vmem((NZ - 1, rows, BLOCK), BF16),
            vmem((NZ - 1, nr, nc - BLOCK), BF16),
            vmem((NY, nr, BLOCK), BF16),
            vmem((nr, nc), F32),
            vmem((NZ - 1, nr, nc - BLOCK), BF16),
            vmem((NY - 1, nr, BLOCK), BF16),
            vmem((NY, NZ, nc // BLOCK, nr, BLOCK), BF16),
            vmem((4, 8, BLOCK), F32),
            vmem((17, 8, BLOCK), F32),
            dma((3, NY)), dma((14,)), dma((14,)),
            dma((NZ,)), dma((NZ - 1,)), dma((NZ - 1,)), dma((NZ - 1,)),
        ],
        compiler_params=pltpu.CompilerParams(
            collective_id=0, has_side_effects=True, vmem_limit_bytes=32 * 1024 * 1024
        ),
        name="synchronise",
    )(*[pltpu.with_memory_space_constraint(a, pltpu.HBM) for a in (outer_params, local_params, momentum)])


    parts = 8
    return pl.pallas_call(
        outer_step,
        out_shape=[
            jax.ShapeDtypeStruct((rows, cols), F32),
            jax.ShapeDtypeStruct((rows, cols), F32),
            jax.ShapeDtypeStruct((cols // BLOCK, rows), F32),
        ],
        in_specs=[pl.BlockSpec(memory_space=pltpu.VMEM)] * 5,
        out_specs=[pl.BlockSpec(memory_space=pltpu.HBM)] * 3,
        scratch_shapes=[
            vmem((parts, rows // parts, cols), F32),
            vmem((parts, rows // parts, cols), F32),
            dma((2 * parts + 1,)),
        ],
        compiler_params=pltpu.CompilerParams(vmem_limit_bytes=8 * 1024 * 1024),
        name="outer_step",
    )(*outs)


def solution(mesh):
    finer = Mesh(mesh.devices.reshape([SIZES[a] for a in AXES]), AXES)
    placed = (P(SHARD, None), P(REPLICA, SHARD, None), P(SHARD, None))
    return jax.shard_map(
        per_device,
        mesh=finer,
        in_specs=placed,
        out_specs=(P(SHARD, None), P(SHARD, None), P(None, SHARD)),
        check_vma=False,
    )
```

```python
import jax
import jax.numpy as jnp
from jax import lax
from jax.experimental import pallas as pl
from jax.experimental.pallas import tpu as pltpu
from jax.sharding import Mesh
from jax.sharding import PartitionSpec as P

F32, BF16 = jnp.float32, jnp.bfloat16
MESH = pl.DeviceIdType.MESH
BLOCK = 128
AXES = ("y", "z", "x", "core")
SIZES = {"y": 4, "z": 8, "x": 4, "core": 2}
REPLICA = ("y", "z")
SHARD = ("x", "core")
NY, NZ = SIZES["y"], SIZES["z"]
WORKERS = NY * NZ

epsilon = 1e-06
clip_level = 0.5
outer_rate = 0.7
outer_decay = 0.9
grid_levels = 7.0

CURVE = (
    6.579723256002266,
    -12.987145762286145,
    12.194590761626122,
    -6.583999071997054,
    1.9907873039801487,
)

Y_STEPS = (2, 1, 3)
Z_FAR = (4, 3, 5, 2, 6, 1, 7)
Z_NEAR = (1, 7, 2, 6, 3, 5, 4)
CELL = tuple((a, b) for a in range(4) for b in range(2) if (a, b) != (0, 0))


def curve(r):
    t = r * r
    p = CURVE[-1]
    for c in CURVE[-2::-1]:
        p = p * t + c
    return (r * t) * p


def smooth_round(v):
    whole = jnp.round(v)
    return whole + curve(curve(v - whole))


def eighth_power(s):
    t = s * s
    return (s * jnp.abs(s)) * t * (t * t)


def eighth_root(c):
    c = c.astype(F32)
    size = jnp.exp2(0.125 * jnp.log2(jnp.maximum(jnp.abs(c), 1e-37)))
    return jnp.where(c < 0.0, -size, size)


def kernel(
    outer_hbm, local_hbm, momentum_hbm, gradient_ref, factor_ref, scales_ref, outer_v, momentum_v,
    local_v, maxima, maxima_y, max_own, maxima_z, max_all,
    inverse, inverse_z, spread, raw_y, raw_z, partial, partial_y, total, parts_z, parts_y, gathered,
    squares, squares_in, load_sem, one_s, one_r, raw_r, gz_r, gy_r, gh_r,
):
    y, z = lax.axis_index("y"), lax.axis_index("z")
    x, core = lax.axis_index("x"), lax.axis_index("core")
    at = {"y": y, "z": z, "x": x, "core": core}
    rows, cols = outer_v.shape
    nr, nc = rows // NY, cols // NZ
    per = nc // BLOCK
    near = per - 1
    nb = cols // BLOCK
    entry_count = rows * cols * SIZES["x"] * SIZES["core"]
    lane = lax.broadcasted_iota(jnp.int32, (8, BLOCK), 1)
    MY, MZ, MA, RY, RZ, PZ, PY, GZ, GO, GY, GH, QC, QY, QZ = range(14)

    def peer(**steps):
        return {k: lax.rem(at[k] + s, SIZES[k]) for k, s in steps.items()}

    def send(src, dst, ss, rs, **steps):
        pltpu.make_async_remote_copy(
            src_ref=src, dst_ref=dst, send_sem=ss, recv_sem=rs,
            device_id=peer(**steps), device_id_type=MESH,
        ).start()

    def all_of(ref, ss, rs):
        return pltpu.make_async_remote_copy(
            src_ref=ref, dst_ref=ref, send_sem=ss, recv_sem=rs,
            device_id=peer(y=1), device_id_type=MESH,
        )

    def landed(ref, sem):
        all_of(ref, one_s.at[0], sem).wait_recv()

    def row_of(g):
        return pl.ds(pl.multiple_of(g * nr, nr), nr)

    def aligned(n, count=1):
        return pl.ds(pl.multiple_of(n * BLOCK, BLOCK), count * BLOCK)

    load_momentum = pltpu.make_async_copy(momentum_hbm, momentum_v, load_sem.at[2, 0])
    loads = [
        pltpu.make_async_copy(src.at[pl.ds(g * nr, nr)], dst.at[pl.ds(g * nr, nr)], load_sem.at[k, g])
        for g in range(NY)
        for k, (src, dst) in enumerate(((local_hbm.at[0], local_v), (outer_hbm, outer_v)))
    ]
    for c in loads:
        c.start()

    barrier = pltpu.get_barrier_semaphore()
    friends = (
        [dict(y=s) for s in range(1, NY)]
        + [dict(z=s) for s in range(1, NZ)]
        + [dict(y=a, z=b) for a in range(1, NY) for b in (1, NZ - 1)]
        + [dict(x=a, core=b) for a, b in CELL]
    )
    for f in friends:
        pl.semaphore_signal(barrier, inc=1, device_id=peer(**f), device_id_type=MESH)

    lasts = jnp.zeros((8, BLOCK), F32)
    for g in range(NY):
        loads[2 * g].wait()
        loads[2 * g + 1].wait()

        def block_max(p, acc, g=g):
            out, lasts = acc
            for j in range(per):
                for r in range(nr // 8):
                    where = (pl.ds(g * nr + r * 8, 8), aligned(p * per + j))
                    deltas = outer_v[where] - local_v[where].astype(F32)
                    most = jnp.max(jnp.abs(deltas), axis=1, keepdims=True)
                    out = jnp.where(lane == r * nb + p * per + j, most, out)
                    if j == near:
                        lasts = jnp.where(lane == p * (rows // 8) + g * (nr // 8) + r, most, lasts)
            return out, lasts

        maxima[g], lasts = lax.fori_loop(
            0, NZ, block_max, (jnp.zeros((8, BLOCK), F32), lasts), unroll=4
        )
    maxima[NY] = lasts

    load_momentum.start()
    pl.semaphore_wait(barrier, len(friends))

    order = (4, 3, 5, 2, 6, 1, 7, 0)
    pieces = [lax.rem(z + o, NZ) for o in order]

    def send_raw_y(i):
        for k, s in enumerate(Y_STEPS):
            send(
                local_v.at[row_of(lax.rem(y + s, NY)), aligned(pieces[i] * per, near)],
                raw_y.at[k, i], one_s.at[RY], raw_r.at[i], y=s,
            )

    def send_raw_z(i):
        s = Z_FAR[i]
        send(
            local_v.at[:, aligned(lax.rem(z + s, NZ) * per + near)],
            raw_z.at[i], one_s.at[RZ], one_r.at[RZ], z=s,
        )

    for i, s in enumerate(Y_STEPS):
        send(maxima.at[lax.rem(y + s, NY)], maxima_y.at[i, 0], one_s.at[MY], one_r.at[MY], y=s)
        send(maxima.at[NY], maxima_y.at[i, 1], one_s.at[MY], one_r.at[MY], y=s)
    for i in range(NZ):
        send_raw_y(i)
        if i < 3:
            send_raw_z(i)
    landed(maxima_y, one_r.at[MY])
    for k, row in enumerate((y, NY)):
        m = maxima[row]
        for i in range(len(Y_STEPS)):
            m = jnp.maximum(m, maxima_y[i, k])
        max_own[k] = m
    for i, s in enumerate(Z_FAR):
        send(max_own, maxima_z.at[i], one_s.at[MZ], one_r.at[MZ], z=s)
    for i in range(3, NZ - 1):
        send_raw_z(i)
    landed(maxima_z, one_r.at[MZ])
    m, lasts = max_own[0], max_own[1]
    for i in range(len(Z_FAR)):
        m = jnp.maximum(m, maxima_z[i, 0])
        lasts = jnp.maximum(lasts, maxima_z[i, 1])
    max_all[y] = m
    for s in Y_STEPS:
        send(max_all.at[y], max_all.at[y], one_s.at[MA], one_r.at[MA], y=s)

    inverse_scale = grid_levels / (m + epsilon)
    for b in range(nb):
        for r in range(nr // 8):
            n = r * nb + b
            inverse[b, pl.ds(r * 8, 8), :] = jnp.broadcast_to(
                inverse_scale[:, n : n + 1], (8, BLOCK)
            )

    def encoded(o, local, inv):
        v = (o - local.astype(F32)) * inv
        return smooth_round(v).astype(BF16).astype(F32)

    def along_y(i):
        p = pieces[i]
        landed(raw_y.at[:, i], raw_r.at[i])

        def encode(j, _):
            lanes = aligned(j)
            columns = aligned(p * per + j)
            o = outer_v[row_of(y), columns]
            inv = inverse[p * per + j]
            acc = encoded(o, local_v[row_of(y), columns], inv)
            for k in range(len(Y_STEPS)):
                acc += encoded(o, raw_y[k, i, :, lanes], inv)
            if i < NZ - 1:
                partial[i, :, lanes] = eighth_power(acc).astype(BF16)
            else:
                total[:, lanes] = acc
            return 0

        lax.fori_loop(0, near, encode, 0, unroll=True)
        if i < NZ - 1:
            send(partial.at[i], parts_z.at[i], one_s.at[PZ], one_r.at[PZ], z=order[i])

    def along_z():
        landed(raw_z, one_r.at[RZ])
        last = z * per + near
        turned = pltpu.roll(grid_levels / (lasts + epsilon), BLOCK - z * (rows // 8), 1)
        for r in range(rows // 8):
            inverse_z[pl.ds(r * 8, 8), :] = jnp.broadcast_to(turned[:, r : r + 1], (8, BLOCK))

        def encode(g, _):
            inv = inverse_z[row_of(g), :]
            o = outer_v[row_of(g), aligned(last)]
            acc = encoded(o, local_v[row_of(g), aligned(last)], inv)
            for k in range(NZ - 1):
                acc += encoded(o, raw_z[k, row_of(g), :], inv)
            partial_y[g] = eighth_power(acc).astype(BF16)

            @pl.when(g == y)
            def _():
                total[:, pl.ds(near * BLOCK, BLOCK)] = acc

            return 0

        lax.fori_loop(0, NY, encode, 0, unroll=2)
        for k, s in enumerate(Y_STEPS):
            send(partial_y.at[lax.rem(y + s, NY)], parts_y.at[k], one_s.at[PY], one_r.at[PY], y=s)

    for i in range(5):
        along_y(i)
    along_z()
    for i in range(5, NZ):
        along_y(i)
    landed(maxima_y.at[:, 0], one_r.at[MA])
    def spread_scale(g):
        group_scale = (max_all[g] + epsilon) * (1.0 / (grid_levels * WORKERS))
        for b in range(nb):
            for r in range(nr // 8):
                n = r * nb + b
                spread[b, pl.ds(g * nr + r * 8, 8), :] = jnp.broadcast_to(
                    group_scale[:, n : n + 1], (8, BLOCK)
                )

    for g in range(NY):
        spread_scale(g)

    stack = []
    for g in range(NY):
        for r in range(nr // 8):
            turned = max_all[g] if r == 0 else pltpu.roll(max_all[g], BLOCK - r * nb, 1)
            stack.append(turned)
    scales_ref[...] = jnp.concatenate(stack, axis=0).T[:nb]

    landed(parts_z, one_r.at[PZ])
    landed(parts_y, one_r.at[PY])

    sq = jnp.zeros((8, BLOCK), F32)
    for j in range(per):
        lanes = pl.ds(j * BLOCK, BLOCK)
        acc = total[:, lanes]
        if j < near:
            for i in range(NZ - 1):
                acc += eighth_root(parts_z[i, :, lanes])
        else:
            for i in range(NY - 1):
                acc += eighth_root(parts_y[i])
        gathered[y, z, j] = eighth_power(acc).astype(BF16)
        g = acc / inverse[z * per + j] * (1.0 / WORKERS)
        g2 = g * g
        for r in range(nr // 8):
            sq += g2[r * 8 : r * 8 + 8]
    squares[0] = sq

    most = pl.ds(0, near)

    def pass_on(i):
        source = lax.rem(z + NZ - Z_NEAR[i], NZ)
        ref = gathered.at[y, source, most]
        landed(ref, gz_r.at[i])
        if i >= 2:
            for s in Y_STEPS:
                send(ref, ref, one_s.at[GY], gy_r.at[i], y=s)

    def pass_last(i):
        ref = gathered.at[:, z, near]
        send(ref, ref, one_s.at[GH], gh_r.at[i], z=Z_FAR[i])

    def add_up(slot, first, count, sem):
        landed(squares_in.at[pl.ds(first, count)], sem)
        acc = squares[slot]
        for i in range(count):
            acc += squares_in[first + i]
        squares[slot + 1] = acc

    for i, s in enumerate(Z_NEAR):
        send(squares.at[0], squares_in.at[i], one_s.at[QZ], one_r.at[QZ], z=s)
    ref = gathered.at[y, z, most]
    for i in reversed(range(2, NZ - 1)):
        send(ref, ref, one_s.at[GZ], gz_r.at[i], z=Z_NEAR[i])
    ref = gathered.at[y, z]
    for s in Y_STEPS:
        send(ref, ref, one_s.at[GO], one_r.at[GO], y=s)
    ref = gathered.at[y, z, most]
    for i in range(2):
        for s in Y_STEPS:
            send(ref, ref, one_s.at[GY], gy_r.at[i], y=s, z=Z_NEAR[i])
    for i in range(2):
        send(ref, ref, one_s.at[GZ], gz_r.at[i], z=Z_NEAR[i])

    landed(raw_z.at[pl.ds(0, NY - 1)], one_r.at[GO])
    add_up(0, 0, 7, one_r.at[QZ])
    for i, s in enumerate(Y_STEPS):
        send(squares.at[1], squares_in.at[7 + i], one_s.at[QY], one_r.at[QY], y=s)
    pass_on(2)
    pass_on(3)
    for i in range(NZ - 1):
        pass_last(i)
    pass_on(4)
    pass_on(5)
    pass_on(6)
    add_up(1, 7, 3, one_r.at[QY])
    for i, (a, b) in enumerate(CELL):
        send(squares.at[2], squares_in.at[10 + i], one_s.at[QC], one_r.at[QC], x=a, core=b)

    pass_on(0)
    pass_on(1)

    for i in range(NZ):
        source = z if i == 0 else lax.rem(z + NZ - Z_NEAR[i - 1], NZ)
        if i > 0:
            landed(raw_y.at[:, 0], gy_r.at[i - 1])
            landed(gathered.at[:, source, near], gh_r.at[Z_FAR.index(Z_NEAR[i - 1])])

        def decode(group, _, source=source):
            for j in range(per):
                sums = eighth_root(gathered[group, source, j])
                gradient_ref[row_of(group), aligned(source * per + j)] = (
                    sums * spread[source * per + j, row_of(group)]
                )
            return 0

        lax.fori_loop(0, NY, decode, 0, unroll=True)

    load_momentum.wait()
    add_up(2, 10, 7, one_r.at[QC])
    square_total = jnp.sum(squares[3], axis=(0, 1), keepdims=True)
    root_mean = jnp.sqrt(square_total / entry_count + epsilon)
    factor_ref[...] = jnp.broadcast_to(jnp.minimum(1.0, clip_level / root_mean), (8, BLOCK))

    for ref, n in (
        (maxima_y, MY), (maxima_z, MZ), (maxima_y.at[:, 0], MA), (raw_y, RY), (raw_z, RZ), (parts_z, PZ),
        (parts_y, PY), (parts_z, GZ), (raw_z.at[pl.ds(0, NY - 1)], GO),
        (raw_y.at[:, pl.ds(0, NZ - 1)], GY), (raw_z, GH), (squares_in.at[pl.ds(0, 7)], QC),
        (squares_in.at[pl.ds(7, 3)], QY), (squares_in.at[pl.ds(10, 7)], QZ),
    ):
        all_of(ref, one_s.at[n], one_r.at[n]).wait_send()


def outer_step(
    gradient_ref, factor_ref, scales_ref, outer_ref, momentum_ref,
    params_hbm, momentum_hbm, scales_hbm, params_v, momentum_v, sem,
):
    parts, part = params_v.shape[0], params_v.shape[1]
    copies = [pltpu.make_async_copy(scales_ref, scales_hbm, sem.at[2 * parts])]
    copies[0].start()
    factor = factor_ref[0:1, 0:1]
    for i in range(parts):
        where = pl.ds(i * part, part)
        clipped = factor * gradient_ref[where]
        after = outer_decay * momentum_ref[where] + clipped
        momentum_v[i] = after
        params_v[i] = outer_ref[where] - outer_rate * (clipped + outer_decay * after)
        for k, (src, dst) in enumerate(((params_v, params_hbm), (momentum_v, momentum_hbm))):
            copies.append(pltpu.make_async_copy(src.at[i], dst.at[where], sem.at[2 * i + k]))
            copies[-1].start(priority=k)
    for c in copies:
        c.wait()


def per_device(outer_params, local_params, momentum):
    rows, cols = outer_params.shape
    nr, nc = rows // NY, cols // NZ
    vmem = pltpu.VMEM
    dma = pltpu.SemaphoreType.DMA
    outs = pl.pallas_call(
        kernel,
        out_shape=(
            jax.ShapeDtypeStruct((rows, cols), F32),
            jax.ShapeDtypeStruct((8, BLOCK), F32),
            jax.ShapeDtypeStruct((cols // BLOCK, rows), F32),
            jax.ShapeDtypeStruct((rows, cols), F32),
            jax.ShapeDtypeStruct((rows, cols), F32),
        ),
        in_specs=[pl.BlockSpec(memory_space=pltpu.HBM)] * 3,
        out_specs=[pl.BlockSpec(memory_space=pltpu.VMEM)] * 5,
        scratch_shapes=[
            vmem((rows, cols), BF16),
            vmem((NY + 1, 8, BLOCK), F32),
            vmem((NY - 1, 2, 8, BLOCK), F32),
            vmem((2, 8, BLOCK), F32),
            vmem((NZ - 1, 2, 8, BLOCK), F32),
            vmem((NY, 8, BLOCK), F32),
            vmem((cols // BLOCK, nr, BLOCK), F32),
            vmem((rows, BLOCK), F32),
            vmem((cols // BLOCK, rows, BLOCK), F32),
            vmem((NY - 1, NZ, nr, nc - BLOCK), BF16),
            vmem((NZ - 1, rows, BLOCK), BF16),
            vmem((NZ - 1, nr, nc - BLOCK), BF16),
            vmem((NY, nr, BLOCK), BF16),
            vmem((nr, nc), F32),
            vmem((NZ - 1, nr, nc - BLOCK), BF16),
            vmem((NY - 1, nr, BLOCK), BF16),
            vmem((NY, NZ, nc // BLOCK, nr, BLOCK), BF16),
            vmem((4, 8, BLOCK), F32),
            vmem((17, 8, BLOCK), F32),
            dma((3, NY)), dma((14,)), dma((14,)),
            dma((NZ,)), dma((NZ - 1,)), dma((NZ - 1,)), dma((NZ - 1,)),
        ],
        compiler_params=pltpu.CompilerParams(
            collective_id=0, has_side_effects=True, vmem_limit_bytes=32 * 1024 * 1024
        ),
        name="synchronise",
    )(*[pltpu.with_memory_space_constraint(a, pltpu.HBM) for a in (outer_params, local_params, momentum)])


    parts = 8
    return pl.pallas_call(
        outer_step,
        out_shape=[
            jax.ShapeDtypeStruct((rows, cols), F32),
            jax.ShapeDtypeStruct((rows, cols), F32),
            jax.ShapeDtypeStruct((cols // BLOCK, rows), F32),
        ],
        in_specs=[pl.BlockSpec(memory_space=pltpu.VMEM)] * 5,
        out_specs=[pl.BlockSpec(memory_space=pltpu.HBM)] * 3,
        scratch_shapes=[
            vmem((parts, rows // parts, cols), F32),
            vmem((parts, rows // parts, cols), F32),
            dma((2 * parts + 1,)),
        ],
        compiler_params=pltpu.CompilerParams(vmem_limit_bytes=8 * 1024 * 1024),
        name="outer_step",
    )(*outs)


def solution(mesh):
    finer = Mesh(mesh.devices.reshape([SIZES[a] for a in AXES]), AXES)
    placed = (P(SHARD, None), P(REPLICA, SHARD, None), P(SHARD, None))
    return jax.shard_map(
        per_device,
        mesh=finer,
        in_specs=placed,
        out_specs=(P(SHARD, None), P(SHARD, None), P(None, SHARD)),
        check_vma=False,
    )
```
